256 devices in a mesh: blk: 64 (over x, y_hi, z), rep: 4 (over y_lo, core).
Axes of the slice: x: 4, y: 4 (y_hi: 2, y_lo: 2; y = y_hi * 2 + y_lo), z: 8, core: 2. Of those that a mesh axis runs over, the one named last changes fastest.
Arguments:
- embeddings: float32 [131072, 768], P(('blk', 'rep')), may hold values from -6 to 6
- ranks: int32 [131072], replicated, may hold values from 0 to 131071, each once
Outputs:
- earlier_best: float32 [131072], P(('blk', 'rep'))
- later_best: float32 [131072], P(('blk', 'rep'))
The draws below stay inside these ranges and needn't reach their ends.
Inputs may be any that keep to these rules, and one draw needn't show every extreme that they name: ranks is a permutation of 0 .. 131071.
All inputs are finite; a program needn't handle non-finite values.
Results may differ from the reference program's by a relative error of at most 0.0012.
Values may be sent and summed in bfloat16 or wider, within the bound.
A program may use at most 64 MiB of HBM per device.

```python
import jax
import jax.numpy as jnp
from jax import lax

D = 768
STEPS = 3
BLOCK = 2048
N = 131072
N_BLK = 64


def levels(rng, shape, cuts, low, top_value):
    def one(position, blocks):
        steps = jax.random.uniform(jax.random.fold_in(jax.random.fold_in(rng, 6), position), (blocks,), jnp.float32, low / len(cuts), top_value / len(cuts))
        return jnp.repeat(jnp.exp(steps), shape[position] // blocks).reshape((-1,) + (1,) * (len(shape) - position - 1))

    level = one(*cuts[0])
    for cut in cuts[1:]:
        level = level * one(*cut)
    return level


def noise(own_key, shape, spread, reach, shards=(), held_as=jnp.bfloat16):
    array = spread * jax.random.normal(own_key, shape, jnp.float32)
    if shards:
        array = array * levels(own_key, shape, shards, -0.22, 0.18)
    return jnp.clip(array, -reach, reach).astype(held_as)


def setup_inputs(seed: int = 0) -> dict:
    arg_keys = jax.random.split(jax.random.key(seed), 3)
    embeddings = noise(arg_keys[0], (N, D), 1.0, 6.0, ((0, 256),), jnp.float32)
    ranks = jax.random.permutation(arg_keys[1], N).astype(jnp.int32)
    return dict(embeddings=embeddings, ranks=ranks)


def reference(embeddings, ranks):
    squares = lax.optimization_barrier(jnp.sum(embeddings * embeddings, axis=1, keepdims=True))
    unit = (embeddings * lax.rsqrt(squares + 1e-06)).astype(jnp.bfloat16).astype(jnp.float32)
    units = unit.reshape(N_BLK, BLOCK, D)
    ordered = ranks.reshape(N_BLK, BLOCK)

    def one_block(index):
        host = units[index]
        host_rank = ordered[index]
        row_best = jnp.full((BLOCK,), -1.0, jnp.float32)
        columns = []
        for offset in range(STEPS + 1):
            other = (index - offset) % N_BLK
            scores = jnp.dot(host, units[other].T, precision=lax.Precision.HIGHEST, preferred_element_type=jnp.float32)
            kept = jnp.where(ordered[other][None, :] < host_rank[:, None], scores, jnp.float32(-1.0))
            row_best = jnp.maximum(row_best, lax.optimization_barrier(jnp.max(kept, axis=1)))
            columns.append(lax.optimization_barrier(jnp.max(kept, axis=0)))
        return (row_best, jnp.stack(columns))
    row_best, column_best = lax.map(one_block, jnp.arange(N_BLK, dtype=jnp.int32))
    later = column_best[:, 0]
    for offset in range(1, STEPS + 1):
        later = jnp.maximum(later, jnp.roll(column_best[:, offset], -offset, axis=0))
    return (row_best.reshape(N), later.reshape(N))
```

```python
import functools

import jax
import jax.numpy as jnp
from jax import lax
from jax.experimental import pallas as pl
from jax.experimental.pallas import tpu as pltpu

MESH = pl.DeviceIdType.MESH
ROWS = 512
WIDTH = 768
CHUNKS = 8
PIECE = ROWS // CHUNKS
HALF = CHUNKS // 2
TILE = 256
LOW = -1.0

UP, UP2, DOWN, FAR, SIDE, PAIR, PAIR_SIDE, PAIR_DOWN, PAIR_FAR = range(9)


def kernel(
    blocks,
    emb_hbm,
    rank_hbm,
    early_ref,
    late_ref,
    emb,
    raw,
    host,
    visit,
    lane_rank,
    row_rank,
    host_best,
    visit_best,
    host_out,
    host_in,
    visit_out,
    visit_in,
    load_sem,
    rank_sem,
    send_sem,
    recv_sem,
    out_send,
    out_recv,
):
    b = lax.axis_index("blk")
    r = lax.axis_index("rep")
    y, c = r // 2, r % 2
    next_b, next_y = (b + 1) % blocks, (y + (b % 8) // 7) % 2
    prev_b, prev_y = (b + blocks - 1) % blocks, (y + (7 - b % 8) // 7) % 2
    back_b = (b + blocks - 2) % blocks
    back_y = (prev_y + (7 - prev_b % 8) // 7) % 2
    up = (next_b, next_y * 2 + c)
    down = (prev_b, prev_y * 2 + c)
    back = (back_b, back_y * 2 + c)
    side = (b, (1 - y) * 2 + c)
    pair = (b, y * 2 + 1 - c)

    def part(base_y, slot):
        return ((base_y + slot % 2) % 2) * 2 + (c + slot // 2) % 2

    def rows(i):
        return pl.ds(i * PIECE, PIECE)

    def copy(stream, i):
        own = host.at[0, rows(i)]
        mine_far = host.at[0, pl.ds(ROWS + i * PIECE, PIECE)]
        next_own = host.at[1, rows(i)]
        next_far = host.at[1, pl.ds(ROWS + i * PIECE, PIECE)]
        if stream == UP:
            src, dst, to = own, visit.at[0, rows(i)], up
        elif stream == UP2:
            src, dst, to = visit.at[0, rows(i)], visit.at[1, rows(i)], up
        elif stream == DOWN:
            src, dst, to = own, next_own, down
        elif stream == FAR and i < HALF:
            src, dst, to = next_own, next_far, side
        elif stream == FAR:
            src, dst, to = mine_far, next_far, down
        elif stream == SIDE:
            src, dst, to = own, mine_far, side
        elif stream == PAIR:
            src, dst, to = own, host.at[0, pl.ds(2 * ROWS + i * PIECE, PIECE)], pair
        elif stream == PAIR_SIDE:
            src, dst, to = mine_far, host.at[0, pl.ds(3 * ROWS + i * PIECE, PIECE)], pair
        elif stream == PAIR_DOWN:
            src, dst, to = next_own, host.at[1, pl.ds(2 * ROWS + i * PIECE, PIECE)], pair
        else:
            src, dst, to = next_far, host.at[1, pl.ds(3 * ROWS + i * PIECE, PIECE)], pair
        return pltpu.make_async_remote_copy(
            src_ref=src,
            dst_ref=dst,
            send_sem=send_sem.at[stream, i],
            recv_sem=recv_sem.at[stream, i],
            device_id=to,
            device_id_type=MESH,
        )

    started = []

    def send(stream, i):
        one = copy(stream, i)
        one.start()
        started.append(one)

    def arrived(stream, i):
        copy(stream, i).wait_recv()

    loads = [
        pltpu.make_async_copy(emb_hbm.at[rows(i)], emb.at[rows(i)], load_sem.at[i])
        for i in range(CHUNKS)
    ]
    for load in loads:
        load.start()
    rank_loads = [
        pltpu.make_async_copy(
            rank_hbm.at[pl.ds(pl.multiple_of(at * 16, 16), 16)], raw.at[k], rank_sem.at[k]
        )
        for k, at in enumerate((b, next_b, prev_b, back_b))
    ]
    for load in rank_loads:
        load.start()

    barrier = pltpu.get_barrier_semaphore()
    for to in (up, down, side, pair):
        pl.semaphore_signal(barrier, inc=1, device_id=to, device_id_type=MESH)

    host_best[...] = jnp.full_like(host_best, LOW)
    visit_best[...] = jnp.full_like(visit_best, LOW)

    def first(i):
        for stream in (UP, DOWN, SIDE, PAIR):
            send(stream, i)

    for i in range(CHUNKS):
        loads[i].wait()
        x = emb[rows(i), :]
        squares = jnp.sum(x * x, axis=1, keepdims=True)
        host[0, rows(i), :] = (x * lax.rsqrt(squares + 1e-06)).astype(jnp.bfloat16)
        if i == 0:
            pl.semaphore_wait(barrier, 4)
        else:
            first(i - 1)
    for load in rank_loads:
        load.wait()
    first(CHUNKS - 1)

    for k, base_y in ((0, y), (1, next_y)):
        for slot in range(4):
            lane_rank[k, pl.ds(slot * 4, 4), :] = raw[
                k, pl.ds(part(base_y, slot) * 4, 4), :
            ].astype(jnp.float32)
    for k, (at, base_y) in enumerate(((0, y), (2, prev_y), (3, back_y))):
        for t in range(4):
            line = raw[at, pl.ds(part(base_y, 0) * 4 + t, 1), :].astype(jnp.float32)
            row_rank[k, pl.ds(t * 128, 128), :] = jnp.broadcast_to(line, (128, 128)).T

    def meet(k, first_tile, tiles, who, start, count):
        source = host.at[0, pl.ds(0, ROWS)] if who == 0 else visit.at[who - 1]

        def one(j, carry):
            at = pl.multiple_of(j * TILE, TILE)
            scores = lax.dot_general(
                source[pl.ds(start, count), :],
                host[k, pl.ds(at, TILE), :],
                (((1,), (1,)), ((), ())),
                preferred_element_type=jnp.float32,
            )
            below = row_rank[who, pl.ds(start, count), :]
            best = visit_best[who, pl.ds(start, count), :]
            for t in range(TILE // 128):
                above = lane_rank[k, pl.ds(j * (TILE // 128) + t, 1), :]
                kept = jnp.where(below < above, scores[:, t * 128 : (t + 1) * 128], LOW)
                best = jnp.maximum(best, kept)
                over = jnp.max(kept.reshape(count // 8, 8, 128), axis=0)
                where = pl.ds(pl.multiple_of(at + t * 128, 128), 128)
                host_best[k, :, where] = jnp.maximum(host_best[k, :, where], over)
            visit_best[who, pl.ds(start, count), :] = best
            return carry

        lax.fori_loop(first_tile, first_tile + tiles, one, 0)

    meet(0, 0, 2, 0, 0, ROWS)
    for i in range(CHUNKS):
        arrived(PAIR, i)
    meet(0, 4, 2, 0, 0, ROWS)
    for i in range(CHUNKS):
        arrived(SIDE, i)
        send(PAIR_SIDE, i)
        arrived(DOWN, i)
        send(PAIR_DOWN, i)
        if i < HALF:
            send(FAR, i)
        arrived(UP, i)
        send(UP2, i)
        if i >= HALF:
            send(FAR, i)
        if i == HALF - 1:
            meet(0, 2, 1, 0, 0, ROWS)
        if i == HALF:
            for n in range(HALF):
                arrived(PAIR_SIDE, n)
            meet(0, 6, 1, 0, 0, ROWS)
    for i in range(HALF, CHUNKS):
        arrived(PAIR_SIDE, i)
    for i in range(CHUNKS):
        arrived(PAIR_DOWN, i)
    for i in range(HALF):
        arrived(FAR, i)
        send(PAIR_FAR, i)
        arrived(FAR, i + HALF)
        send(PAIR_FAR, i + HALF)
        if i == 0:
            meet(0, 3, 1, 0, 0, ROWS)
            meet(0, 7, 1, 0, 0, ROWS)
        else:
            meet(0, (i - 1) * 3, 3 if i < 3 else 2, 1, 0, ROWS)
    meet(1, 0, 2, 1, 0, ROWS)
    meet(1, 4, 2, 1, 0, ROWS)
    for i in range(CHUNKS):
        arrived(PAIR_FAR, i)
    meet(1, 2, 2, 1, 0, ROWS)
    meet(1, 6, 2, 1, 0, ROWS)

    def host_result(k):
        for n in range(16):
            host_out[k, n // 4, pl.ds(n % 4, 1), :] = jnp.max(
                host_best[k, :, pl.ds(n * 128, 128)], axis=0, keepdims=True
            )

    def visit_result(who):
        for t in range(4):
            visit_out[who, pl.ds(t, 1), :] = jnp.max(
                visit_best[who, pl.ds(t * 128, 128), :].T, axis=0, keepdims=True
            )

    def host_copy(k, slot):
        return pltpu.make_async_remote_copy(
            src_ref=host_out.at[k, slot],
            dst_ref=host_in.at[k, slot],
            send_sem=out_send.at[k * 4 + slot],
            recv_sem=out_recv.at[k * 4 + slot],
            device_id=(b, part(y, slot)) if k == 0 else (next_b, part(next_y, slot)),
            device_id_type=MESH,
        )

    def visit_copy(who):
        return pltpu.make_async_remote_copy(
            src_ref=visit_out.at[who],
            dst_ref=visit_in.at[who],
            send_sem=out_send.at[8 + who],
            recv_sem=out_recv.at[8 + who],
            device_id=down if who == 1 else back,
            device_id_type=MESH,
        )

    results = []

    def give(one):
        one.start()
        results.append(one)

    host_result(0)
    visit_result(1)
    visit_result(0)
    for slot in range(1, 4):
        give(host_copy(0, slot))
    give(visit_copy(1))

    for i in range(HALF):
        arrived(UP2, i)
    meet(1, 0, 8, 2, 0, HALF * PIECE)
    for i in range(HALF, CHUNKS):
        arrived(UP2, i)
        meet(1, 0, 8, 2, i * PIECE, PIECE)
    host_result(1)
    visit_result(2)
    for slot in range(4):
        give(host_copy(1, slot))
    give(visit_copy(2))

    for one in started:
        one.wait_send()
    for one in results:
        one.wait_recv()
    early = host_out[0, 0]
    for slot in range(1, 4):
        early = jnp.maximum(early, host_in[0, slot])
    for slot in range(4):
        early = jnp.maximum(early, host_in[1, slot])
    early_ref[...] = early
    late_ref[...] = jnp.maximum(visit_out[0], jnp.maximum(visit_in[1], visit_in[2]))
    for one in results:
        one.wait_send()


def shards(blocks, embeddings, ranks):
    out = jax.ShapeDtypeStruct((4, 128), jnp.float32)
    early, late = pl.pallas_call(
        functools.partial(kernel, blocks),
        out_shape=(out, out),
        in_specs=[pl.BlockSpec(memory_space=pl.ANY)] * 2,
        out_specs=(pl.BlockSpec(memory_space=pltpu.VMEM),) * 2,
        scratch_shapes=[
            pltpu.VMEM((ROWS, WIDTH), jnp.float32),
            pltpu.VMEM((4, 16, 128), jnp.int32),
            pltpu.VMEM((2, 4 * ROWS, WIDTH), jnp.bfloat16),
            pltpu.VMEM((2, ROWS, WIDTH), jnp.bfloat16),
            pltpu.VMEM((2, 16, 128), jnp.float32),
            pltpu.VMEM((3, ROWS, 128), jnp.float32),
            pltpu.VMEM((2, 8, 4 * ROWS), jnp.float32),
            pltpu.VMEM((3, ROWS, 128), jnp.float32),
            pltpu.VMEM((2, 4, 4, 128), jnp.float32),
            pltpu.VMEM((2, 4, 4, 128), jnp.float32),
            pltpu.VMEM((3, 4, 128), jnp.float32),
            pltpu.VMEM((3, 4, 128), jnp.float32),
            pltpu.SemaphoreType.DMA((CHUNKS,)),
            pltpu.SemaphoreType.DMA((4,)),
            pltpu.SemaphoreType.DMA((9, CHUNKS)),
            pltpu.SemaphoreType.DMA((9, CHUNKS)),
            pltpu.SemaphoreType.DMA((11,)),
            pltpu.SemaphoreType.DMA((11,)),
        ],
        compiler_params=pltpu.CompilerParams(
            collective_id=0, has_side_effects=True, vmem_limit_bytes=40 << 20
        ),
    )(embeddings, ranks.reshape(-1, 128))
    return early.reshape(-1), late.reshape(-1)


def solution(mesh):
    from jax.sharding import PartitionSpec as P

    return jax.shard_map(
        functools.partial(shards, mesh.shape["blk"]),
        mesh=mesh,
        in_specs=(P(("blk", "rep"), None), P()),
        out_specs=(P(("blk", "rep")), P(("blk", "rep"))),
        check_vma=False,
    )
```

```python
import functools

import jax
import jax.numpy as jnp
from jax import lax
from jax.experimental import pallas as pl
from jax.experimental.pallas import tpu as pltpu

MESH = pl.DeviceIdType.MESH
ROWS = 512
WIDTH = 768
CHUNKS = 8
PIECE = ROWS // CHUNKS
HALF = CHUNKS // 2
TILE = 256
LOW = -1.0

UP, UP2, DOWN, FAR, SIDE, PAIR, PAIR_SIDE, PAIR_DOWN, PAIR_FAR = range(9)


def kernel(
    blocks,
    emb_hbm,
    rank_hbm,
    early_ref,
    late_ref,
    emb,
    raw,
    host,
    visit,
    lane_rank,
    row_rank,
    host_best,
    visit_best,
    host_out,
    host_in,
    visit_out,
    visit_in,
    load_sem,
    rank_sem,
    send_sem,
    recv_sem,
    out_send,
    out_recv,
):
    b = lax.axis_index("blk")
    r = lax.axis_index("rep")
    y, c = r // 2, r % 2
    next_b, next_y = (b + blocks - 1) % blocks, (y + (7 - b % 8) // 7) % 2
    prev_b, prev_y = (b + 1) % blocks, (y + (b % 8) // 7) % 2
    back_b, back_y = (b + 2) % blocks, (prev_y + (prev_b % 8) // 7) % 2
    up = (next_b, next_y * 2 + c)
    down = (prev_b, prev_y * 2 + c)
    back = (back_b, back_y * 2 + c)
    side = (b, (1 - y) * 2 + c)
    pair = (b, y * 2 + 1 - c)

    def part(base_y, slot):
        return ((base_y + slot % 2) % 2) * 2 + (c + slot // 2) % 2

    def rows(i):
        return pl.ds(i * PIECE, PIECE)

    def copy(stream, i):
        own = host.at[0, rows(i)]
        mine_far = host.at[0, pl.ds(ROWS + i * PIECE, PIECE)]
        next_own = host.at[1, rows(i)]
        next_far = host.at[1, pl.ds(ROWS + i * PIECE, PIECE)]
        if stream == UP:
            src, dst, to = own, visit.at[0, rows(i)], up
        elif stream == UP2:
            src, dst, to = visit.at[0, rows(i)], visit.at[1, rows(i)], up
        elif stream == DOWN:
            src, dst, to = own, next_own, down
        elif stream == FAR and i < HALF:
            src, dst, to = next_own, next_far, side
        elif stream == FAR:
            src, dst, to = mine_far, next_far, down
        elif stream == SIDE:
            src, dst, to = own, mine_far, side
        elif stream == PAIR:
            src, dst, to = own, host.at[0, pl.ds(2 * ROWS + i * PIECE, PIECE)], pair
        elif stream == PAIR_SIDE:
            src, dst, to = mine_far, host.at[0, pl.ds(3 * ROWS + i * PIECE, PIECE)], pair
        elif stream == PAIR_DOWN:
            src, dst, to = next_own, host.at[1, pl.ds(2 * ROWS + i * PIECE, PIECE)], pair
        else:
            src, dst, to = next_far, host.at[1, pl.ds(3 * ROWS + i * PIECE, PIECE)], pair
        return pltpu.make_async_remote_copy(
            src_ref=src,
            dst_ref=dst,
            send_sem=send_sem.at[stream, i],
            recv_sem=recv_sem.at[stream, i],
            device_id=to,
            device_id_type=MESH,
        )

    started = []

    def send(stream, i):
        one = copy(stream, i)
        one.start()
        started.append(one)

    def arrived(stream, i):
        copy(stream, i).wait_recv()

    loads = [
        pltpu.make_async_copy(emb_hbm.at[rows(i)], emb.at[rows(i)], load_sem.at[i])
        for i in range(CHUNKS)
    ]
    for load in loads:
        load.start()
    rank_loads = [
        pltpu.make_async_copy(
            rank_hbm.at[pl.ds(pl.multiple_of(at * 16, 16), 16)], raw.at[k], rank_sem.at[k]
        )
        for k, at in enumerate((b, next_b, prev_b, back_b))
    ]
    for load in rank_loads:
        load.start()

    barrier = pltpu.get_barrier_semaphore()
    for to in (up, down, side, pair):
        pl.semaphore_signal(barrier, inc=1, device_id=to, device_id_type=MESH)

    host_best[...] = jnp.full_like(host_best, LOW)
    visit_best[...] = jnp.full_like(visit_best, LOW)

    def first(i):
        for stream in (UP, DOWN, SIDE, PAIR):
            send(stream, i)

    for i in range(CHUNKS):
        loads[i].wait()
        x = emb[rows(i), :]
        squares = jnp.sum(x * x, axis=1, keepdims=True)
        host[0, rows(i), :] = (x * lax.rsqrt(squares + 1e-06)).astype(jnp.bfloat16)
        if i == 0:
            pl.semaphore_wait(barrier, 4)
        else:
            first(i - 1)
    for load in rank_loads:
        load.wait()
    first(CHUNKS - 1)

    for k, base_y in ((0, y), (1, next_y)):
        for slot in range(4):
            lane_rank[k, pl.ds(slot * 4, 4), :] = raw[
                k, pl.ds(part(base_y, slot) * 4, 4), :
            ].astype(jnp.float32)
    for k, (at, base_y) in enumerate(((0, y), (2, prev_y), (3, back_y))):
        for t in range(4):
            line = raw[at, pl.ds(part(base_y, 0) * 4 + t, 1), :].astype(jnp.float32)
            row_rank[k, pl.ds(t * 128, 128), :] = jnp.broadcast_to(line, (128, 128)).T

    def meet(k, first_tile, tiles, who, start, count):
        source = host.at[0, pl.ds(0, ROWS)] if who == 0 else visit.at[who - 1]

        def one(j, carry):
            at = pl.multiple_of(j * TILE, TILE)
            scores = lax.dot_general(
                source[pl.ds(start, count), :],
                host[k, pl.ds(at, TILE), :],
                (((1,), (1,)), ((), ())),
                preferred_element_type=jnp.float32,
            )
            below = row_rank[who, pl.ds(start, count), :]
            best = visit_best[who, pl.ds(start, count), :]
            for t in range(TILE // 128):
                above = lane_rank[k, pl.ds(j * (TILE // 128) + t, 1), :]
                kept = jnp.where(above < below, scores[:, t * 128 : (t + 1) * 128], LOW)
                best = jnp.maximum(best, kept)
                over = jnp.max(kept.reshape(count // 8, 8, 128), axis=0)
                where = pl.ds(pl.multiple_of(at + t * 128, 128), 128)
                host_best[k, :, where] = jnp.maximum(host_best[k, :, where], over)
            visit_best[who, pl.ds(start, count), :] = best
            return carry

        lax.fori_loop(first_tile, first_tile + tiles, one, 0)

    meet(0, 0, 2, 0, 0, ROWS)
    for i in range(CHUNKS):
        arrived(PAIR, i)
    meet(0, 4, 2, 0, 0, ROWS)
    for i in range(CHUNKS):
        arrived(SIDE, i)
        send(PAIR_SIDE, i)
        arrived(DOWN, i)
        send(PAIR_DOWN, i)
        if i < HALF:
            send(FAR, i)
        arrived(UP, i)
        send(UP2, i)
        if i >= HALF:
            send(FAR, i)
        if i == HALF - 1:
            meet(0, 2, 1, 0, 0, ROWS)
        if i == HALF:
            for n in range(HALF):
                arrived(PAIR_SIDE, n)
            meet(0, 6, 1, 0, 0, ROWS)
    for i in range(HALF, CHUNKS):
        arrived(PAIR_SIDE, i)
    for i in range(CHUNKS):
        arrived(PAIR_DOWN, i)
    for i in range(HALF):
        arrived(FAR, i)
        send(PAIR_FAR, i)
        arrived(FAR, i + HALF)
        send(PAIR_FAR, i + HALF)
        if i == 0:
            meet(0, 3, 1, 0, 0, ROWS)
            meet(0, 7, 1, 0, 0, ROWS)
        else:
            meet(0, (i - 1) * 3, 3 if i < 3 else 2, 1, 0, ROWS)
    meet(1, 0, 2, 1, 0, ROWS)
    meet(1, 4, 2, 1, 0, ROWS)
    for i in range(CHUNKS):
        arrived(PAIR_FAR, i)
    meet(1, 2, 2, 1, 0, ROWS)
    meet(1, 6, 2, 1, 0, ROWS)

    def host_result(k):
        for n in range(16):
            host_out[k, n // 4, pl.ds(n % 4, 1), :] = jnp.max(
                host_best[k, :, pl.ds(n * 128, 128)], axis=0, keepdims=True
            )

    def visit_result(who):
        for t in range(4):
            visit_out[who, pl.ds(t, 1), :] = jnp.max(
                visit_best[who, pl.ds(t * 128, 128), :].T, axis=0, keepdims=True
            )

    def host_copy(k, slot):
        return pltpu.make_async_remote_copy(
            src_ref=host_out.at[k, slot],
            dst_ref=host_in.at[k, slot],
            send_sem=out_send.at[k * 4 + slot],
            recv_sem=out_recv.at[k * 4 + slot],
            device_id=(b, part(y, slot)) if k == 0 else (next_b, part(next_y, slot)),
            device_id_type=MESH,
        )

    def visit_copy(who):
        return pltpu.make_async_remote_copy(
            src_ref=visit_out.at[who],
            dst_ref=visit_in.at[who],
            send_sem=out_send.at[8 + who],
            recv_sem=out_recv.at[8 + who],
            device_id=down if who == 1 else back,
            device_id_type=MESH,
        )

    results = []

    def give(one):
        one.start()
        results.append(one)

    host_result(0)
    visit_result(1)
    visit_result(0)
    for slot in range(1, 4):
        give(host_copy(0, slot))
    give(visit_copy(1))

    for i in range(HALF):
        arrived(UP2, i)
    meet(1, 0, 8, 2, 0, HALF * PIECE)
    for i in range(HALF, CHUNKS):
        arrived(UP2, i)
        meet(1, 0, 8, 2, i * PIECE, PIECE)
    host_result(1)
    visit_result(2)
    for slot in range(4):
        give(host_copy(1, slot))
    give(visit_copy(2))

    for one in started:
        one.wait_send()
    for one in results:
        one.wait_recv()
    late = host_out[0, 0]
    for slot in range(1, 4):
        late = jnp.maximum(late, host_in[0, slot])
    for slot in range(4):
        late = jnp.maximum(late, host_in[1, slot])
    late_ref[...] = late
    early_ref[...] = jnp.maximum(visit_out[0], jnp.maximum(visit_in[1], visit_in[2]))
    for one in results:
        one.wait_send()


def shards(blocks, embeddings, ranks):
    out = jax.ShapeDtypeStruct((4, 128), jnp.float32)
    early, late = pl.pallas_call(
        functools.partial(kernel, blocks),
        out_shape=(out, out),
        in_specs=[pl.BlockSpec(memory_space=pltpu.HBM)] * 2,
        out_specs=(pl.BlockSpec(memory_space=pltpu.VMEM),) * 2,
        scratch_shapes=[
            pltpu.VMEM((ROWS, WIDTH), jnp.float32),
            pltpu.VMEM((4, 16, 128), jnp.int32),
            pltpu.VMEM((2, 4 * ROWS, WIDTH), jnp.bfloat16),
            pltpu.VMEM((2, ROWS, WIDTH), jnp.bfloat16),
            pltpu.VMEM((2, 16, 128), jnp.float32),
            pltpu.VMEM((3, ROWS, 128), jnp.float32),
            pltpu.VMEM((2, 8, 4 * ROWS), jnp.float32),
            pltpu.VMEM((3, ROWS, 128), jnp.float32),
            pltpu.VMEM((2, 4, 4, 128), jnp.float32),
            pltpu.VMEM((2, 4, 4, 128), jnp.float32),
            pltpu.VMEM((3, 4, 128), jnp.float32),
            pltpu.VMEM((3, 4, 128), jnp.float32),
            pltpu.SemaphoreType.DMA((CHUNKS,)),
            pltpu.SemaphoreType.DMA((4,)),
            pltpu.SemaphoreType.DMA((9, CHUNKS)),
            pltpu.SemaphoreType.DMA((9, CHUNKS)),
            pltpu.SemaphoreType.DMA((11,)),
            pltpu.SemaphoreType.DMA((11,)),
        ],
        compiler_params=pltpu.CompilerParams(
            collective_id=0, has_side_effects=True, vmem_limit_bytes=40 << 20
        ),
    )(embeddings, ranks.reshape(-1, 128))
    return early.reshape(-1), late.reshape(-1)


def solution(mesh):
    from jax.sharding import PartitionSpec as P

    return jax.shard_map(
        functools.partial(shards, mesh.shape["blk"]),
        mesh=mesh,
        in_specs=(P(("blk", "rep"), None), P()),
        out_specs=(P(("blk", "rep")), P(("blk", "rep"))),
        check_vma=False,
    )
```

```python
import functools

import jax
import jax.numpy as jnp
from jax import lax
from jax.experimental import pallas as pl
from jax.experimental.pallas import tpu as pltpu
from jax.sharding import PartitionSpec as P

MESH = pl.DeviceIdType.MESH
ROWS = 512
WIDTH = 768
PIECES = 8
PIECE = ROWS // PIECES
LANES = 128
CHUNKS = ROWS // LANES
HALF = CHUNKS // 2
LOW = -1.0

VIS, VIS2, UP, FAR, SIDE, PAIR, PAIR_SIDE, PAIR_UP, PAIR_FAR = range(9)


def kernel(
    blocks,
    emb_hbm,
    rank_hbm,
    late_ref,
    early_ref,
    emb,
    raw,
    host,
    visit,
    lane_rank,
    row_rank,
    host_best,
    visit_best,
    host_out,
    host_in,
    visit_out,
    visit_in,
    load_sem,
    rank_sem,
    send_sem,
    recv_sem,
    out_send,
    out_recv,
):
    b = lax.axis_index("blk")
    r = lax.axis_index("rep")
    y, c = r // 2, r % 2
    low_b, low_y = (b + blocks - 1) % blocks, (y + (7 - b % 8) // 7) % 2
    high_b, high_y = (b + 1) % blocks, (y + (b % 8) // 7) % 2
    top_b, top_y = (b + 2) % blocks, (high_y + (high_b % 8) // 7) % 2
    low = (low_b, low_y * 2 + c)
    high = (high_b, high_y * 2 + c)
    top = (top_b, top_y * 2 + c)
    side = (b, (1 - y) * 2 + c)
    pair = (b, y * 2 + 1 - c)

    def part(base_y, slot):
        return ((base_y + slot // 2) % 2) * 2 + (c + slot % 2) % 2

    def rows(i):
        return pl.ds(i * PIECE, PIECE)

    def copy(stream, i):
        if stream == VIS:
            src, dst, to = visit.at[0, rows(i)], visit.at[1, rows(i)], low
        elif stream == VIS2:
            src, dst, to = visit.at[1, rows(i)], visit.at[2, rows(i)], low
        elif stream == UP:
            src, dst, to = host.at[0, i], host.at[1, i], high
        elif stream == FAR and i < HALF:
            src, dst, to = host.at[1, i], host.at[1, 2 * CHUNKS + i], side
        elif stream == FAR:
            src, dst, to = host.at[0, 2 * CHUNKS + i], host.at[1, 2 * CHUNKS + i], high
        elif stream == SIDE:
            src, dst, to = host.at[0, i], host.at[0, 2 * CHUNKS + i], side
        else:
            k = 0 if stream in (PAIR, PAIR_SIDE) else 1
            at = i if stream in (PAIR, PAIR_UP) else 2 * CHUNKS + i
            src, dst, to = host.at[k, at], host.at[k, at + CHUNKS], pair
        return pltpu.make_async_remote_copy(
            src_ref=src,
            dst_ref=dst,
            send_sem=send_sem.at[stream, i],
            recv_sem=recv_sem.at[stream, i],
            device_id=to,
            device_id_type=MESH,
        )

    started = []

    def send(stream, i):
        one = copy(stream, i)
        one.start()
        started.append(one)

    def arrived(stream, i):
        copy(stream, i).wait_recv()

    loads = [
        pltpu.make_async_copy(emb_hbm.at[rows(i)], emb.at[rows(i)], load_sem.at[i])
        for i in range(PIECES)
    ]
    for load in loads:
        load.start()

    barrier = pltpu.get_barrier_semaphore()
    for to in (low, high, side, pair):
        pl.semaphore_signal(barrier, inc=1, device_id=to, device_id_type=MESH)

    rank_loads = [
        pltpu.make_async_copy(
            rank_hbm.at[pl.ds(pl.multiple_of(at * 16, 16), 16)], raw.at[k], rank_sem.at[k]
        )
        for k, at in enumerate((b, low_b, high_b, top_b))
    ]
    for load in rank_loads:
        load.start()

    host_best[...] = jnp.full_like(host_best, LOW)
    visit_best[...] = jnp.full_like(visit_best, LOW)

    def first(j):
        for stream in (UP, SIDE, PAIR):
            send(stream, j)

    for j in range(CHUNKS):
        group = []
        for i in (2 * j, 2 * j + 1):
            loads[i].wait()
            x = emb[rows(i), :]
            squares = jnp.sum(x * x, axis=1, keepdims=True)
            unit = x * lax.rsqrt(squares + 1e-06)
            visit[0, rows(i), :] = unit.astype(jnp.bfloat16)
            group.append(unit)
            if i == 0:
                pl.semaphore_wait(barrier, 4)
            else:
                send(VIS, i - 1)
        host[0, j] = jnp.concatenate(group, axis=0).T.astype(jnp.bfloat16)
        if j:
            first(j - 1)
    send(VIS, PIECES - 1)
    for load in rank_loads:
        load.wait()
    first(CHUNKS - 1)

    for k, base_y in ((0, y), (1, low_y)):
        for slot in range(4):
            lane_rank[k, pl.ds(slot * 4, 4), :] = raw[
                k, pl.ds(part(base_y, slot) * 4, 4), :
            ].astype(jnp.float32)
    for k, (at, base_y) in enumerate(((0, y), (2, high_y), (3, top_y))):
        for t in range(4):
            line = raw[at, pl.ds(part(base_y, 0) * 4 + t, 1), :].astype(jnp.float32)
            row_rank[k, pl.ds(t * 128, 128), :] = jnp.broadcast_to(line, (128, 128)).T

    def meet(k, chunk, chunks, who, start, count):
        scores = jnp.dot(
            visit[who, pl.ds(start, count), :],
            jnp.concatenate([host[k, chunk + n] for n in range(chunks)], axis=1),
            preferred_element_type=jnp.float32,
        )
        after = row_rank[who, pl.ds(start, count), :]
        best = visit_best[who, pl.ds(start, count), :]
        for n in range(chunks):
            before = lane_rank[k, pl.ds(chunk + n, 1), :]
            kept = jnp.where(before < after, scores[:, n * LANES : (n + 1) * LANES], LOW)
            best = jnp.maximum(best, kept)
            over = jnp.max(kept.reshape(count // 8, 8, LANES), axis=0)
            host_best[k, chunk + n] = jnp.maximum(host_best[k, chunk + n], over)
        visit_best[who, pl.ds(start, count), :] = best

    def half(k, which, who, start=0, count=ROWS):
        meet(k, which * 2 * CHUNKS, 2 * CHUNKS, who, start, count)

    def host_result(k):
        for n in range(4 * CHUNKS):
            host_out[k, n // CHUNKS, pl.ds(n % CHUNKS, 1), :] = jnp.max(
                host_best[k, n], axis=0, keepdims=True
            )

    def visit_result(who, t):
        visit_out[who, pl.ds(t, 1), :] = jnp.max(
            visit_best[who, pl.ds(t * 128, 128), :].T, axis=0, keepdims=True
        )

    def host_copy(k, slot):
        return pltpu.make_async_remote_copy(
            src_ref=host_out.at[k, slot],
            dst_ref=host_in.at[k, slot],
            send_sem=out_send.at[k * 4 + slot],
            recv_sem=out_recv.at[k * 4 + slot],
            device_id=(b, part(y, slot)) if k == 0 else (low_b, part(low_y, slot)),
            device_id_type=MESH,
        )

    def visit_copy(who):
        return pltpu.make_async_remote_copy(
            src_ref=visit_out.at[who],
            dst_ref=visit_in.at[who],
            send_sem=out_send.at[8 + who],
            recv_sem=out_recv.at[8 + who],
            device_id=high if who == 1 else top,
            device_id_type=MESH,
        )

    results = []

    def give(one):
        one.start()
        results.append(one)

    for j in range(CHUNKS):
        arrived(PAIR, j)
    half(0, 0, 0)
    for j in range(CHUNKS):
        for i in (2 * j, 2 * j + 1):
            arrived(VIS, i)
            send(VIS2, i)
        arrived(SIDE, j)
        send(PAIR_SIDE, j)
        if j >= HALF:
            send(FAR, j)
        arrived(UP, j)
        send(PAIR_UP, j)
        if j < HALF:
            send(FAR, j)
    half(0, 0, 1)
    for j in range(CHUNKS):
        arrived(PAIR_SIDE, j)
    half(0, 1, 0)
    half(0, 1, 1)
    for j in range(CHUNKS):
        arrived(PAIR_UP, j)
    half(1, 0, 1)
    for j in range(HALF):
        for n in (j, j + HALF):
            arrived(FAR, n)
            send(PAIR_FAR, n)
    host_result(0)
    for t in range(4):
        visit_result(0, t)
    for slot in range(1, 4):
        give(host_copy(0, slot))
    for j in range(CHUNKS):
        arrived(PAIR_FAR, j)
    half(1, 1, 1)
    for t in range(4):
        visit_result(1, t)
    for i in range(PIECES // 2):
        arrived(VIS2, i)
    give(visit_copy(1))
    half(1, 0, 2, 0, ROWS // 2)
    half(1, 1, 2, 0, ROWS // 2)
    for i in (4, 5):
        arrived(VIS2, i)
    half(1, 0, 2, 4 * PIECE, 2 * PIECE)
    half(1, 1, 2, 4 * PIECE, 2 * PIECE)
    for t in range(3):
        visit_result(2, t)
    for i in (6, 7):
        arrived(VIS2, i)
        meet(1, 0, 4 * CHUNKS, 2, i * PIECE, PIECE)
    host_result(1)
    visit_result(2, 3)
    for slot in range(4):
        give(host_copy(1, slot))
    give(visit_copy(2))

    for one in started:
        one.wait_send()
    for one in results:
        one.wait_recv()
    late = host_out[0, 0]
    for slot in range(1, 4):
        late = jnp.maximum(late, host_in[0, slot])
    late_ref[0] = late
    late = host_in[1, 0]
    for slot in range(1, 4):
        late = jnp.maximum(late, host_in[1, slot])
    late_ref[1] = late
    early_ref[0] = jnp.maximum(visit_out[0], visit_in[1])
    early_ref[1] = visit_in[2]
    for one in results:
        one.wait_send()


def shards(blocks, embeddings, ranks):
    out = jax.ShapeDtypeStruct((2, 4, 128), jnp.float32)
    late, early = pl.pallas_call(
        functools.partial(kernel, blocks),
        out_shape=(out, out),
        in_specs=[pl.BlockSpec(memory_space=pltpu.HBM)] * 2,
        out_specs=(pl.BlockSpec(memory_space=pltpu.VMEM),) * 2,
        scratch_shapes=[
            pltpu.VMEM((ROWS, WIDTH), jnp.float32),
            pltpu.VMEM((4, 16, 128), jnp.int32),
            pltpu.VMEM((2, 4 * CHUNKS, WIDTH, LANES), jnp.bfloat16),
            pltpu.VMEM((3, ROWS, WIDTH), jnp.bfloat16),
            pltpu.VMEM((2, 16, 128), jnp.float32),
            pltpu.VMEM((3, ROWS, 128), jnp.float32),
            pltpu.VMEM((2, 4 * CHUNKS, 8, LANES), jnp.float32),
            pltpu.VMEM((3, ROWS, 128), jnp.float32),
            pltpu.VMEM((2, 4, 4, 128), jnp.float32),
            pltpu.VMEM((2, 4, 4, 128), jnp.float32),
            pltpu.VMEM((3, 4, 128), jnp.float32),
            pltpu.VMEM((3, 4, 128), jnp.float32),
            pltpu.SemaphoreType.DMA((PIECES,)),
            pltpu.SemaphoreType.DMA((4,)),
            pltpu.SemaphoreType.DMA((9, PIECES)),
            pltpu.SemaphoreType.DMA((9, PIECES)),
            pltpu.SemaphoreType.DMA((11,)),
            pltpu.SemaphoreType.DMA((11,)),
        ],
        compiler_params=pltpu.CompilerParams(
            collective_id=0, has_side_effects=True, vmem_limit_bytes=67043328 - (256 << 10)
        ),
    )(embeddings, ranks.reshape(-1, 128))

    def higher(one, other):
        return (jnp.maximum(one[0], other[0]), jnp.maximum(one[1], other[1]))

    start = jnp.float32(LOW)
    late, early = lax.reduce(
        (late.reshape(2, -1), early.reshape(2, -1)), (start, start), higher, (0,)
    )
    return early, late


def solution(mesh):
    return jax.shard_map(
        functools.partial(shards, mesh.shape["blk"]),
        mesh=mesh,
        in_specs=(P(("blk", "rep"), None), P()),
        out_specs=(P(("blk", "rep")), P(("blk", "rep"))),
        check_vma=False,
    )
```

```python
import functools

import jax
import jax.numpy as jnp
from jax import lax
from jax.experimental import pallas as pl
from jax.experimental.pallas import tpu as pltpu
from jax.sharding import PartitionSpec as P

MESH = pl.DeviceIdType.MESH
ROWS = 512
WIDTH = 768
PIECES = 8
PIECE = ROWS // PIECES
LANES = 128
CHUNKS = ROWS // LANES
HALF = CHUNKS // 2
LOW = -1.0

VIS, VIS2, UP, FAR, SIDE, PAIR, PAIR_SIDE, PAIR_UP, PAIR_FAR = range(9)


def kernel(
    blocks,
    emb_hbm,
    rank_hbm,
    early_ref,
    late_ref,
    emb,
    raw,
    host,
    visit,
    lane_rank,
    row_rank,
    host_best,
    visit_best,
    host_out,
    host_in,
    visit_out,
    visit_in,
    load_sem,
    rank_sem,
    send_sem,
    recv_sem,
    ready,
    out_send,
    out_recv,
):
    b = lax.axis_index("blk")
    r = lax.axis_index("rep")
    y, c = r // 2, r % 2
    next_b, next_y = (b + 1) % blocks, (y + (b % 8) // 7) % 2
    prev_b, prev_y = (b + blocks - 1) % blocks, (y + (7 - b % 8) // 7) % 2
    back_b, back_y = (b + blocks - 2) % blocks, (prev_y + (7 - prev_b % 8) // 7) % 2
    ahead = (next_b, next_y * 2 + c)
    behind = (prev_b, prev_y * 2 + c)
    back = (back_b, back_y * 2 + c)
    side = (b, (1 - y) * 2 + c)
    pair = (b, y * 2 + 1 - c)

    def part(base_y, slot):
        return ((base_y + slot // 2) % 2) * 2 + (c + slot % 2) % 2

    def rows(i):
        return pl.ds(i * PIECE, PIECE)

    def copy(stream, i):
        if stream == VIS:
            src, dst, to = visit.at[0, rows(i)], visit.at[1, rows(i)], ahead
        elif stream == VIS2:
            src, dst, to = visit.at[1, rows(i)], visit.at[2, rows(i)], ahead
        elif stream == UP:
            src, dst, to = host.at[0, i], host.at[1, i], behind
        elif stream == FAR and i < HALF:
            src, dst, to = host.at[1, i], host.at[1, 2 * CHUNKS + i], side
        elif stream == FAR:
            src, dst, to = host.at[0, 2 * CHUNKS + i], host.at[1, 2 * CHUNKS + i], behind
        elif stream == SIDE:
            src, dst, to = host.at[0, i], host.at[0, 2 * CHUNKS + i], side
        else:
            k = 0 if stream in (PAIR, PAIR_SIDE) else 1
            at = i if stream in (PAIR, PAIR_UP) else 2 * CHUNKS + i
            src, dst, to = host.at[k, at], host.at[k, at + CHUNKS], pair
        return pltpu.make_async_remote_copy(
            src_ref=src,
            dst_ref=dst,
            send_sem=send_sem.at[stream, i],
            recv_sem=recv_sem.at[stream, i],
            device_id=to,
            device_id_type=MESH,
        )

    started = []

    def send(stream, i):
        one = copy(stream, i)
        one.start()
        started.append(one)

    def arrived(stream, i):
        copy(stream, i).wait_recv()

    loads = [
        pltpu.make_async_copy(emb_hbm.at[rows(i)], emb.at[rows(i)], load_sem.at[i])
        for i in range(PIECES)
    ]
    for load in loads:
        load.start()

    barrier = pltpu.get_barrier_semaphore()
    for to in (behind, side, pair):
        pl.semaphore_signal(barrier, inc=1, device_id=to, device_id_type=MESH)

    rank_loads = [
        pltpu.make_async_copy(
            rank_hbm.at[pl.ds(pl.multiple_of(at * 16, 16), 16)], raw.at[k], rank_sem.at[k]
        )
        for k, at in enumerate((b, next_b, prev_b, back_b))
    ]
    for load in rank_loads:
        load.start()

    host_best[...] = jnp.full_like(host_best, LOW)
    visit_best[...] = jnp.full_like(visit_best, LOW)

    def first(j):
        for stream in (SIDE, PAIR):
            send(stream, j)

    for j in range(CHUNKS):
        group = []
        for i in (2 * j, 2 * j + 1):
            loads[i].wait()
            x = emb[rows(i), :]
            squares = jnp.sum(x * x, axis=1, keepdims=True)
            unit = x * lax.rsqrt(squares + 1e-06)
            visit[0, rows(i), :] = unit.astype(jnp.bfloat16)
            group.append(unit)
            if i == 0:
                pl.semaphore_wait(barrier, 3)
                pl.semaphore_signal(ready, inc=1, device_id=ahead, device_id_type=MESH)
            else:
                send(VIS, i - 1)
        host[0, j] = jnp.concatenate(group, axis=0).T.astype(jnp.bfloat16)
        if j:
            first(j - 1)
    send(VIS, PIECES - 1)
    for load in rank_loads:
        load.wait()
    first(CHUNKS - 1)
    for k, base_y in ((0, y), (1, next_y)):
        for slot in range(4):
            lane_rank[k, pl.ds(slot * 4, 4), :] = raw[
                k, pl.ds(part(base_y, slot) * 4, 4), :
            ].astype(jnp.float32)
    for k, (at, base_y) in enumerate(((0, y), (2, prev_y), (3, back_y))):
        for t in range(4):
            line = raw[at, pl.ds(part(base_y, 0) * 4 + t, 1), :].astype(jnp.float32)
            row_rank[k, pl.ds(t * 128, 128), :] = jnp.broadcast_to(line, (128, 128)).T

    pl.semaphore_wait(ready, 1)
    for j in range(CHUNKS):
        send(UP, j)

    def meet(k, chunk, chunks, who, start, count):
        scores = jnp.dot(
            visit[who, pl.ds(start, count), :],
            jnp.concatenate([host[k, chunk + n] for n in range(chunks)], axis=1),
            preferred_element_type=jnp.float32,
        )
        before = row_rank[who, pl.ds(start, count), :]
        best = visit_best[who, pl.ds(start, count), :]
        for n in range(chunks):
            after = lane_rank[k, pl.ds(chunk + n, 1), :]
            kept = jnp.where(before < after, scores[:, n * LANES : (n + 1) * LANES], LOW)
            best = jnp.maximum(best, kept)
            over = jnp.max(kept.reshape(count // 8, 8, LANES), axis=0)
            host_best[k, chunk + n] = jnp.maximum(host_best[k, chunk + n], over)
        visit_best[who, pl.ds(start, count), :] = best

    def half(k, which, who, start=0, count=ROWS):
        meet(k, which * 2 * CHUNKS, 2 * CHUNKS, who, start, count)

    def host_result(k):
        for n in range(4 * CHUNKS):
            host_out[k, n // CHUNKS, pl.ds(n % CHUNKS, 1), :] = jnp.max(
                host_best[k, n], axis=0, keepdims=True
            )

    def visit_result(who, t):
        visit_out[who, pl.ds(t, 1), :] = jnp.max(
            visit_best[who, pl.ds(t * 128, 128), :].T, axis=0, keepdims=True
        )

    def host_copy(k, slot):
        return pltpu.make_async_remote_copy(
            src_ref=host_out.at[k, slot],
            dst_ref=host_in.at[k, slot],
            send_sem=out_send.at[k * 4 + slot],
            recv_sem=out_recv.at[k * 4 + slot],
            device_id=(b, part(y, slot)) if k == 0 else (next_b, part(next_y, slot)),
            device_id_type=MESH,
        )

    def visit_copy(who):
        return pltpu.make_async_remote_copy(
            src_ref=visit_out.at[who],
            dst_ref=visit_in.at[who],
            send_sem=out_send.at[8 + who],
            recv_sem=out_recv.at[8 + who],
            device_id=behind if who == 1 else back,
            device_id_type=MESH,
        )

    results = []

    def give(one):
        one.start()
        results.append(one)

    for j in range(CHUNKS):
        arrived(PAIR, j)
    half(0, 0, 0)
    for j in range(CHUNKS):
        for i in (2 * j, 2 * j + 1):
            arrived(VIS, i)
            send(VIS2, i)
        arrived(SIDE, j)
        send(PAIR_SIDE, j)
        if j >= HALF:
            send(FAR, j)
        arrived(UP, j)
        send(PAIR_UP, j)
        if j < HALF:
            send(FAR, j)
    half(0, 0, 1)
    for j in range(CHUNKS):
        arrived(PAIR_SIDE, j)
    half(0, 1, 0)
    half(0, 1, 1)
    for j in range(CHUNKS):
        arrived(PAIR_UP, j)
    half(1, 0, 1)
    for j in range(HALF):
        for n in (j, j + HALF):
            arrived(FAR, n)
            send(PAIR_FAR, n)
    host_result(0)
    for t in range(4):
        visit_result(0, t)
    for slot in range(1, 4):
        give(host_copy(0, slot))
    for j in range(CHUNKS):
        arrived(PAIR_FAR, j)
    half(1, 1, 1)
    for t in range(4):
        visit_result(1, t)
    for i in range(PIECES // 2):
        arrived(VIS2, i)
    give(visit_copy(1))
    half(1, 0, 2, 0, ROWS // 2)
    half(1, 1, 2, 0, ROWS // 2)
    for i in (4, 5):
        arrived(VIS2, i)
    half(1, 0, 2, 4 * PIECE, 2 * PIECE)
    half(1, 1, 2, 4 * PIECE, 2 * PIECE)
    for t in range(3):
        visit_result(2, t)
    for i in (6, 7):
        arrived(VIS2, i)
        meet(1, 0, 4 * CHUNKS, 2, i * PIECE, PIECE)
    host_result(1)
    visit_result(2, 3)
    for slot in range(4):
        give(host_copy(1, slot))
    give(visit_copy(2))

    for one in started:
        one.wait_send()
    for one in results:
        one.wait_recv()
    early = host_out[0, 0]
    for slot in range(1, 4):
        early = jnp.maximum(early, host_in[0, slot])
    early_ref[0] = early
    early = host_in[1, 0]
    for slot in range(1, 4):
        early = jnp.maximum(early, host_in[1, slot])
    early_ref[1] = early
    late_ref[0] = jnp.maximum(visit_out[0], visit_in[1])
    late_ref[1] = visit_in[2]
    for one in results:
        one.wait_send()


def shards(blocks, embeddings, ranks):
    out = jax.ShapeDtypeStruct((2, 4, 128), jnp.float32)
    early, late = pl.pallas_call(
        functools.partial(kernel, blocks),
        out_shape=(out, out),
        in_specs=[pl.BlockSpec(memory_space=pltpu.HBM)] * 2,
        out_specs=(pl.BlockSpec(memory_space=pltpu.VMEM),) * 2,
        scratch_shapes=[
            pltpu.VMEM((ROWS, WIDTH), jnp.float32),
            pltpu.VMEM((4, 16, 128), jnp.int32),
            pltpu.VMEM((2, 4 * CHUNKS, WIDTH, LANES), jnp.bfloat16),
            pltpu.VMEM((3, ROWS, WIDTH), jnp.bfloat16),
            pltpu.VMEM((2, 16, 128), jnp.float32),
            pltpu.VMEM((3, ROWS, 128), jnp.float32),
            pltpu.VMEM((2, 4 * CHUNKS, 8, LANES), jnp.float32),
            pltpu.VMEM((3, ROWS, 128), jnp.float32),
            pltpu.VMEM((2, 4, 4, 128), jnp.float32),
            pltpu.VMEM((2, 4, 4, 128), jnp.float32),
            pltpu.VMEM((3, 4, 128), jnp.float32),
            pltpu.VMEM((3, 4, 128), jnp.float32),
            pltpu.SemaphoreType.DMA((PIECES,)),
            pltpu.SemaphoreType.DMA((4,)),
            pltpu.SemaphoreType.DMA((9, PIECES)),
            pltpu.SemaphoreType.DMA((9, PIECES)),
            pltpu.SemaphoreType.REGULAR,
            pltpu.SemaphoreType.DMA((11,)),
            pltpu.SemaphoreType.DMA((11,)),
        ],
        compiler_params=pltpu.CompilerParams(
            collective_id=0, has_side_effects=True, vmem_limit_bytes=54976 << 10
        ),
    )(embeddings, ranks.reshape(-1, 128))

    def higher(one, other):
        return (jnp.maximum(one[0], other[0]), jnp.maximum(one[1], other[1]))

    start = jnp.float32(LOW)
    return lax.reduce(
        (early.reshape(2, -1), late.reshape(2, -1)), (start, start), higher, (0,)
    )


def solution(mesh):
    return jax.shard_map(
        functools.partial(shards, mesh.shape["blk"]),
        mesh=mesh,
        in_specs=(P(("blk", "rep"), None), P()),
        out_specs=(P(("blk", "rep")), P(("blk", "rep"))),
        check_vma=False,
    )
```

```python
import functools

import jax
import jax.numpy as jnp
from jax import lax
from jax.experimental import pallas as pl
from jax.experimental.pallas import tpu as pltpu
from jax.sharding import PartitionSpec as P

MESH = pl.DeviceIdType.MESH
ROWS = 512
WIDTH = 768
SIZES = (64, 192, 128, 128)
ENDS = tuple(sum(SIZES[: i + 1]) for i in range(len(SIZES)))
PIECES = len(SIZES)
EARLY = max(1, sum(end <= 256 for end in ENDS))
LOAD = 64
LANES = 128
CHUNKS = ROWS // LANES
TILES = ROWS // 128
NEAR = 3
LOW = -1.0

VIS, VIS2, UP, FAR, SIDE, PAIR, PAIR_SIDE, PAIR_UP, PAIR_FAR = range(9)


def kernel(
    blocks,
    emb_hbm,
    rank_hbm,
    early_ref,
    late_ref,
    emb,
    raw,
    host,
    visit,
    lane_rank,
    row_rank,
    host_best,
    visit_best,
    host_out,
    host_in,
    visit_out,
    visit_in,
    load_sem,
    rank_sem,
    send_sem,
    recv_sem,
    ready,
    out_send,
    out_recv,
):
    b = lax.axis_index("blk")
    r = lax.axis_index("rep")
    y, c = r // 2, r % 2
    next_b, next_y = (b + 1) % blocks, (y + (b % 8) // 7) % 2
    prev_b, prev_y = (b + blocks - 1) % blocks, (y + (7 - b % 8) // 7) % 2
    back_b, back_y = (b + blocks - 2) % blocks, (prev_y + (7 - prev_b % 8) // 7) % 2
    ahead = (next_b, next_y * 2 + c)
    behind = (prev_b, prev_y * 2 + c)
    back = (back_b, back_y * 2 + c)
    side = (b, (1 - y) * 2 + c)
    pair = (b, y * 2 + 1 - c)

    def part(base_y, slot):
        return ((base_y + slot // 2) % 2) * 2 + (c + slot % 2) % 2

    def rows(i):
        return pl.ds(ENDS[i] - SIZES[i], SIZES[i])

    def copy(stream, i):
        if stream == VIS:
            src, dst, to = visit.at[0, rows(i)], visit.at[1, rows(i)], ahead
        elif stream == VIS2:
            src, dst, to = visit.at[1, rows(i)], visit.at[2, rows(i)], ahead
        elif stream == UP:
            src, dst, to = host.at[0, i], host.at[1, i], behind
        elif stream == FAR and i < NEAR:
            src, dst, to = host.at[1, i], host.at[1, 2 * CHUNKS + i], side
        elif stream == FAR:
            src, dst, to = host.at[0, 2 * CHUNKS + i], host.at[1, 2 * CHUNKS + i], behind
        elif stream == SIDE:
            src, dst, to = host.at[0, i], host.at[0, 2 * CHUNKS + i], side
        else:
            k = 0 if stream in (PAIR, PAIR_SIDE) else 1
            at = i if stream in (PAIR, PAIR_UP) else 2 * CHUNKS + i
            src, dst, to = host.at[k, at], host.at[k, at + CHUNKS], pair
        return pltpu.make_async_remote_copy(
            src_ref=src,
            dst_ref=dst,
            send_sem=send_sem.at[stream, i],
            recv_sem=recv_sem.at[stream, i],
            device_id=to,
            device_id_type=MESH,
        )

    started = []

    def send(stream, i):
        one = copy(stream, i)
        one.start()
        started.append(one)

    def arrived(stream, i):
        copy(stream, i).wait_recv()

    loads = [
        pltpu.make_async_copy(emb_hbm.at[at], emb.at[at], load_sem.at[i])
        for i, at in enumerate(pl.ds(n, LOAD) for n in range(0, ROWS, LOAD))
    ]
    for load in loads:
        load.start()

    barrier = pltpu.get_barrier_semaphore()
    for to in (behind, side, pair):
        pl.semaphore_signal(barrier, inc=1, device_id=to, device_id_type=MESH)

    rank_loads = [
        pltpu.make_async_copy(
            rank_hbm.at[pl.ds(pl.multiple_of(at * 16, 16), 16)], raw.at[k], rank_sem.at[k]
        )
        for k, at in enumerate((b, next_b, prev_b, back_b))
    ]
    for load in rank_loads:
        load.start()

    host_best[...] = jnp.full_like(host_best, LOW)
    visit_best[...] = jnp.full_like(visit_best, LOW)

    def first(j):
        for stream in (SIDE, PAIR):
            send(stream, j)

    for j in range(CHUNKS):
        group = []
        for at in range(j * LANES, (j + 1) * LANES, LOAD):
            loads[at // LOAD].wait()
            x = emb[pl.ds(at, LOAD), :]
            squares = jnp.sum(x * x, axis=1, keepdims=True)
            unit = x * lax.rsqrt(squares + 1e-06)
            visit[0, pl.ds(at, LOAD), :] = unit.astype(jnp.bfloat16)
            group.append(unit)
            if at == 0:
                pl.semaphore_wait(barrier, 3)
                pl.semaphore_signal(ready, inc=1, device_id=ahead, device_id_type=MESH)
            if at in ENDS:
                send(VIS, ENDS.index(at))
        host[0, j] = jnp.concatenate(group, axis=0).T.astype(jnp.bfloat16)
        if j:
            first(j - 1)
    send(VIS, PIECES - 1)
    for load in rank_loads:
        load.wait()
    first(CHUNKS - 1)
    for k, base_y in ((0, y), (1, next_y)):
        for slot in range(4):
            lane_rank[k, pl.ds(slot * 4, 4), :] = raw[
                k, pl.ds(part(base_y, slot) * 4, 4), :
            ].astype(jnp.float32)
    for k, (at, base_y) in enumerate(((0, y), (2, prev_y), (3, back_y))):
        for t in range(4):
            line = raw[at, pl.ds(part(base_y, 0) * 4 + t, 1), :].astype(jnp.float32)
            row_rank[k, pl.ds(t * 128, 128), :] = jnp.broadcast_to(line, (128, 128)).T

    pl.semaphore_wait(ready, 1)
    for j in range(CHUNKS):
        send(UP, j)

    def meet(k, chunk, chunks, who, start, count):
        scores = jnp.dot(
            visit[who, pl.ds(start, count), :],
            jnp.concatenate([host[k, chunk + n] for n in range(chunks)], axis=1),
            preferred_element_type=jnp.float32,
        )
        before = row_rank[who, pl.ds(start, count), :]
        best = visit_best[who, pl.ds(start, count), :]
        for n in range(chunks * LANES // 128):
            at = chunk * LANES // 128 + n
            after = lane_rank[k, pl.ds(at, 1), :]
            kept = jnp.where(before < after, scores[:, n * 128 : (n + 1) * 128], LOW)
            best = jnp.maximum(best, kept)
            over = jnp.max(kept.reshape(count // 8, 8, 128), axis=0)
            host_best[k, at] = jnp.maximum(host_best[k, at], over)
        visit_best[who, pl.ds(start, count), :] = best

    def half(k, which, who, start=0, count=ROWS):
        meet(k, which * 2 * CHUNKS, 2 * CHUNKS, who, start, count)

    def host_result(k):
        for n in range(4 * TILES):
            host_out[k, n // TILES, pl.ds(n % TILES, 1), :] = jnp.max(
                host_best[k, n], axis=0, keepdims=True
            )

    def visit_result(who, t):
        visit_out[who, pl.ds(t, 1), :] = jnp.max(
            visit_best[who, pl.ds(t * 128, 128), :].T, axis=0, keepdims=True
        )

    def host_copy(k, slot):
        return pltpu.make_async_remote_copy(
            src_ref=host_out.at[k, slot],
            dst_ref=host_in.at[k, slot],
            send_sem=out_send.at[k * 4 + slot],
            recv_sem=out_recv.at[k * 4 + slot],
            device_id=(b, part(y, slot)) if k == 0 else (next_b, part(next_y, slot)),
            device_id_type=MESH,
        )

    def visit_copy(who):
        return pltpu.make_async_remote_copy(
            src_ref=visit_out.at[who],
            dst_ref=visit_in.at[who],
            send_sem=out_send.at[8 + who],
            recv_sem=out_recv.at[8 + who],
            device_id=behind if who == 1 else back,
            device_id_type=MESH,
        )

    results = []

    def give(one):
        one.start()
        results.append(one)

    for j in range(CHUNKS):
        arrived(PAIR, j)
    half(0, 0, 0)
    for j in range(CHUNKS):
        for i in range(PIECES):
            if j * LANES < ENDS[i] <= (j + 1) * LANES:
                arrived(VIS, i)
                send(VIS2, i)
        arrived(SIDE, j)
        send(PAIR_SIDE, j)
        if j >= NEAR:
            send(FAR, j)
        arrived(UP, j)
        send(PAIR_UP, j)
        if j < NEAR:
            send(FAR, j)
    half(0, 0, 1)
    for j in range(CHUNKS):
        arrived(PAIR_SIDE, j)
    half(0, 1, 0)
    half(0, 1, 1)
    for j in range(CHUNKS):
        arrived(PAIR_UP, j)
    half(1, 0, 1)
    for j in (0, *range(NEAR, CHUNKS), *range(1, NEAR)):
        arrived(FAR, j)
        send(PAIR_FAR, j)
        if j == 1:
            for i in range(EARLY):
                arrived(VIS2, i)
            half(1, 0, 2, 0, ENDS[EARLY - 1])
    host_result(0)
    for t in range(4):
        visit_result(0, t)
    for slot in range(1, 4):
        give(host_copy(0, slot))
    before_last = ENDS[PIECES - 2]
    for i in range(EARLY, PIECES - 1):
        arrived(VIS2, i)
        half(1, 0, 2, ENDS[i - 1], SIZES[i])
    for j in range(CHUNKS):
        arrived(PAIR_FAR, j)
    half(1, 1, 1)
    for t in range(4):
        visit_result(1, t)
    give(visit_copy(1))
    half(1, 1, 2, 0, before_last)
    for t in range(before_last // 128):
        visit_result(2, t)
    arrived(VIS2, PIECES - 1)
    half(1, 0, 2, before_last, ROWS - before_last)
    half(1, 1, 2, before_last, ROWS - before_last)
    host_result(1)
    for slot in range(4):
        give(host_copy(1, slot))
    for t in range(before_last // 128, 4):
        visit_result(2, t)
    give(visit_copy(2))

    for one in started:
        one.wait_send()
    for one in results[:4]:
        one.wait_recv()
    early = host_out[0, 0]
    for slot in range(1, 4):
        early = jnp.maximum(early, host_in[0, slot])
    early_ref[0] = early
    late_ref[0] = jnp.maximum(visit_out[0], visit_in[1])
    for one in results[4:]:
        one.wait_recv()
    late_ref[1] = visit_in[2]
    early = host_in[1, 0]
    for slot in range(1, 4):
        early = jnp.maximum(early, host_in[1, slot])
    early_ref[1] = early
    for one in results:
        one.wait_send()


def shards(blocks, embeddings, ranks):
    out = jax.ShapeDtypeStruct((2, 4, 128), jnp.float32)
    early, late = pl.pallas_call(
        functools.partial(kernel, blocks),
        out_shape=(out, out),
        in_specs=[pl.BlockSpec(memory_space=pltpu.HBM)] * 2,
        out_specs=(pl.BlockSpec(memory_space=pltpu.VMEM),) * 2,
        scratch_shapes=[
            pltpu.VMEM((ROWS, WIDTH), jnp.float32),
            pltpu.VMEM((4, 16, 128), jnp.int32),
            pltpu.VMEM((2, 4 * CHUNKS, WIDTH, LANES), jnp.bfloat16),
            pltpu.VMEM((3, ROWS, WIDTH), jnp.bfloat16),
            pltpu.VMEM((2, 16, 128), jnp.float32),
            pltpu.VMEM((3, ROWS, 128), jnp.float32),
            pltpu.VMEM((2, 4 * TILES, 8, 128), jnp.float32),
            pltpu.VMEM((3, ROWS, 128), jnp.float32),
            pltpu.VMEM((2, 4, 4, 128), jnp.float32),
            pltpu.VMEM((2, 4, 4, 128), jnp.float32),
            pltpu.VMEM((3, 4, 128), jnp.float32),
            pltpu.VMEM((3, 4, 128), jnp.float32),
            pltpu.SemaphoreType.DMA((ROWS // LOAD,)),
            pltpu.SemaphoreType.DMA((4,)),
            pltpu.SemaphoreType.DMA((9, max(PIECES, CHUNKS))),
            pltpu.SemaphoreType.DMA((9, max(PIECES, CHUNKS))),
            pltpu.SemaphoreType.REGULAR,
            pltpu.SemaphoreType.DMA((11,)),
            pltpu.SemaphoreType.DMA((11,)),
        ],
        compiler_params=pltpu.CompilerParams(
            collective_id=0, has_side_effects=True, vmem_limit_bytes=54976 << 10
        ),
    )(embeddings, ranks.reshape(-1, 128))

    def higher(one, other):
        return (jnp.maximum(one[0], other[0]), jnp.maximum(one[1], other[1]))

    start = jnp.float32(LOW)
    return lax.reduce(
        (early.reshape(2, -1), late.reshape(2, -1)), (start, start), higher, (0,)
    )


def solution(mesh):
    return jax.shard_map(
        functools.partial(shards, mesh.shape["blk"]),
        mesh=mesh,
        in_specs=(P(("blk", "rep"), None), P()),
        out_specs=(P(("blk", "rep")), P(("blk", "rep"))),
        check_vma=False,
    )
```

```python
import functools

import jax
import jax.numpy as jnp
from jax import lax
from jax.experimental import pallas as pl
from jax.experimental.pallas import tpu as pltpu
from jax.sharding import PartitionSpec as P

MESH = pl.DeviceIdType.MESH
ROWS = 512
WIDTH = 768
SIZES = (64, 192, 128, 128)
ENDS = tuple(sum(SIZES[: i + 1]) for i in range(len(SIZES)))
PIECES = len(SIZES)
EARLY = max(1, sum(end <= 256 for end in ENDS))
LOAD = 64
LANES = 128
CHUNKS = ROWS // LANES
TILES = ROWS // 128
NEAR = 3
LOW = -1.0

VIS, VIS2, UP, FAR, SIDE, PAIR, PAIR_SIDE, PAIR_UP, PAIR_FAR = range(9)


def kernel(
    blocks,
    emb_hbm,
    rank_hbm,
    early_ref,
    late_ref,
    emb,
    raw,
    host,
    visit,
    lane_rank,
    row_rank,
    host_best,
    visit_best,
    host_out,
    host_in,
    visit_out,
    visit_in,
    load_sem,
    rank_sem,
    send_sem,
    recv_sem,
    ready,
    out_send,
    out_recv,
):
    b = lax.axis_index("blk")
    r = lax.axis_index("rep")
    y, c = r // 2, r % 2
    next_b, next_y = (b + 1) % blocks, (y + (b % 8) // 7) % 2
    prev_b, prev_y = (b + blocks - 1) % blocks, (y + (7 - b % 8) // 7) % 2
    back_b, back_y = (b + blocks - 2) % blocks, (prev_y + (7 - prev_b % 8) // 7) % 2
    ahead = (next_b, next_y * 2 + c)
    behind = (prev_b, prev_y * 2 + c)
    back = (back_b, back_y * 2 + c)
    side = (b, (1 - y) * 2 + c)
    pair = (b, y * 2 + 1 - c)

    def part(base_y, slot):
        return ((base_y + slot // 2) % 2) * 2 + (c + slot % 2) % 2

    def rows(i):
        return pl.ds(ENDS[i] - SIZES[i], SIZES[i])

    def copy(stream, i):
        if stream == VIS:
            src, dst, to = visit.at[0, rows(i)], visit.at[1, rows(i)], ahead
        elif stream == VIS2:
            src, dst, to = visit.at[1, rows(i)], visit.at[2, rows(i)], ahead
        elif stream == UP:
            src, dst, to = host.at[0, i], host.at[1, i], behind
        elif stream == FAR and i < NEAR:
            src, dst, to = host.at[1, i], host.at[1, 2 * CHUNKS + i], side
        elif stream == FAR:
            src, dst, to = host.at[0, 2 * CHUNKS + i], host.at[1, 2 * CHUNKS + i], behind
        elif stream == SIDE:
            src, dst, to = host.at[0, i], host.at[0, 2 * CHUNKS + i], side
        else:
            k = 0 if stream in (PAIR, PAIR_SIDE) else 1
            at = i if stream in (PAIR, PAIR_UP) else 2 * CHUNKS + i
            src, dst, to = host.at[k, at], host.at[k, at + CHUNKS], pair
        return pltpu.make_async_remote_copy(
            src_ref=src,
            dst_ref=dst,
            send_sem=send_sem.at[stream, i],
            recv_sem=recv_sem.at[stream, i],
            device_id=to,
            device_id_type=MESH,
        )

    started = []

    def send(stream, i):
        one = copy(stream, i)
        one.start()
        started.append(one)

    def arrived(stream, i):
        copy(stream, i).wait_recv()

    loads = [
        pltpu.make_async_copy(emb_hbm.at[at], emb.at[at], load_sem.at[i])
        for i, at in enumerate(pl.ds(n, LOAD) for n in range(0, ROWS, LOAD))
    ]
    for load in loads:
        load.start()

    barrier = pltpu.get_barrier_semaphore()
    for to in (behind, side, pair):
        pl.semaphore_signal(barrier, inc=1, device_id=to, device_id_type=MESH)

    rank_loads = [
        pltpu.make_async_copy(
            rank_hbm.at[pl.ds(pl.multiple_of(at * 16, 16), 16)], raw.at[k], rank_sem.at[k]
        )
        for k, at in enumerate((b, next_b, prev_b, back_b))
    ]
    for load in rank_loads:
        load.start()

    host_best[...] = jnp.full_like(host_best, LOW)
    visit_best[...] = jnp.full_like(visit_best, LOW)

    def first(j):
        for stream in (SIDE, PAIR):
            send(stream, j)

    for j in range(CHUNKS):
        group = []
        for at in range(j * LANES, (j + 1) * LANES, LOAD):
            loads[at // LOAD].wait()
            x = emb[pl.ds(at, LOAD), :]
            squares = jnp.sum(x * x, axis=1, keepdims=True)
            unit = x * lax.rsqrt(squares + 1e-06)
            visit[0, pl.ds(at, LOAD), :] = unit.astype(jnp.bfloat16)
            group.append(unit)
            if at == 0:
                pl.semaphore_wait(barrier, 3)
                pl.semaphore_signal(ready, inc=1, device_id=ahead, device_id_type=MESH)
            if at in ENDS:
                send(VIS, ENDS.index(at))
        host[0, j] = jnp.concatenate(group, axis=0).T.astype(jnp.bfloat16)
        if j:
            first(j - 1)
    send(VIS, PIECES - 1)
    for load in rank_loads:
        load.wait()
    first(CHUNKS - 1)
    for k, base_y in ((0, y), (1, next_y)):
        for slot in range(4):
            lane_rank[k, pl.ds(slot * 4, 4), :] = raw[
                k, pl.ds(part(base_y, slot) * 4, 4), :
            ].astype(jnp.float32)
    for k, (at, base_y) in enumerate(((0, y), (2, prev_y), (3, back_y))):
        for t in range(4):
            line = raw[at, pl.ds(part(base_y, 0) * 4 + t, 1), :].astype(jnp.float32)
            row_rank[k, pl.ds(t * 128, 128), :] = jnp.broadcast_to(line, (128, 128)).T

    pl.semaphore_wait(ready, 1)
    for j in range(CHUNKS):
        send(UP, j)

    def meet(k, chunk, chunks, who, start, count):
        scores = jnp.dot(
            visit[who, pl.ds(start, count), :],
            jnp.concatenate([host[k, chunk + n] for n in range(chunks)], axis=1),
            preferred_element_type=jnp.float32,
        )
        before = row_rank[who, pl.ds(start, count), :]
        best = visit_best[who, pl.ds(start, count), :]
        for n in range(chunks * LANES // 128):
            at = chunk * LANES // 128 + n
            after = lane_rank[k, pl.ds(at, 1), :]
            kept = jnp.where(before < after, scores[:, n * 128 : (n + 1) * 128], LOW)
            best = jnp.maximum(best, kept)
            over = jnp.max(kept.reshape(count // 8, 8, 128), axis=0)
            host_best[k, at] = jnp.maximum(host_best[k, at], over)
        visit_best[who, pl.ds(start, count), :] = best

    def half(k, which, who, start=0, count=ROWS):
        meet(k, which * 2 * CHUNKS, 2 * CHUNKS, who, start, count)

    def host_result(k, slot):
        for n in range(TILES):
            host_out[k, slot, pl.ds(n, 1), :] = jnp.max(
                host_best[k, slot * TILES + n], axis=0, keepdims=True
            )

    def visit_result(who, t):
        visit_out[who, pl.ds(t, 1), :] = jnp.max(
            visit_best[who, pl.ds(t * 128, 128), :].T, axis=0, keepdims=True
        )

    def host_copy(k, slot):
        return pltpu.make_async_remote_copy(
            src_ref=host_out.at[k, slot],
            dst_ref=host_in.at[k, slot],
            send_sem=out_send.at[k * 4 + slot],
            recv_sem=out_recv.at[k * 4 + slot],
            device_id=(b, part(y, slot)) if k == 0 else (next_b, part(next_y, slot)),
            device_id_type=MESH,
        )

    def visit_copy(who):
        return pltpu.make_async_remote_copy(
            src_ref=visit_out.at[who],
            dst_ref=visit_in.at[who],
            send_sem=out_send.at[8 + who],
            recv_sem=out_recv.at[8 + who],
            device_id=behind if who == 1 else back,
            device_id_type=MESH,
        )

    results = []

    def give(one):
        one.start()
        results.append(one)

    for j in range(CHUNKS):
        arrived(PAIR, j)
    half(0, 0, 0)
    for j in range(CHUNKS):
        for i in range(PIECES):
            if j * LANES < ENDS[i] <= (j + 1) * LANES:
                arrived(VIS, i)
                send(VIS2, i)
        arrived(SIDE, j)
        send(PAIR_SIDE, j)
        if j >= NEAR:
            send(FAR, j)
        arrived(UP, j)
        send(PAIR_UP, j)
        if j < NEAR:
            send(FAR, j)
    half(0, 0, 1)
    for j in range(CHUNKS):
        arrived(PAIR_SIDE, j)
    half(0, 1, 0)
    half(0, 1, 1)
    for j in range(CHUNKS):
        arrived(PAIR_UP, j)
    half(1, 0, 1)
    for j in (0, *range(NEAR, CHUNKS), *range(1, NEAR)):
        arrived(FAR, j)
        send(PAIR_FAR, j)
        if j == 1:
            for i in range(EARLY):
                arrived(VIS2, i)
            half(1, 0, 2, 0, ENDS[EARLY - 1])
    for slot in range(4):
        host_result(0, slot)
    for t in range(4):
        visit_result(0, t)
    for slot in range(1, 4):
        give(host_copy(0, slot))
    before_last = ENDS[PIECES - 2]
    for i in range(EARLY, PIECES - 1):
        arrived(VIS2, i)
        half(1, 0, 2, ENDS[i - 1], SIZES[i])
    for j in range(CHUNKS):
        arrived(PAIR_FAR, j)
    half(1, 1, 1)
    for t in range(4):
        visit_result(1, t)
    give(visit_copy(1))
    half(1, 1, 2, 0, before_last)
    for t in range(before_last // 128):
        visit_result(2, t)
    arrived(VIS2, PIECES - 1)
    for which in (1, 0):
        half(1, which, 2, before_last, ROWS - before_last)
        for slot in (2 * which, 2 * which + 1):
            host_result(1, slot)
        for slot in (2 * which, 2 * which + 1):
            give(host_copy(1, slot))
    for t in range(before_last // 128, 4):
        visit_result(2, t)
    give(visit_copy(2))

    for one in started:
        one.wait_send()
    for one in results[:4]:
        one.wait_recv()
    early = host_out[0, 0]
    for slot in range(1, 4):
        early = jnp.maximum(early, host_in[0, slot])
    early_ref[0] = early
    late_ref[0] = jnp.maximum(visit_out[0], visit_in[1])
    for one in results[4:]:
        one.wait_recv()
    late_ref[1] = visit_in[2]
    early = host_in[1, 0]
    for slot in range(1, 4):
        early = jnp.maximum(early, host_in[1, slot])
    early_ref[1] = early
    for one in results:
        one.wait_send()


def shards(blocks, embeddings, ranks):
    out = jax.ShapeDtypeStruct((2, 4, 128), jnp.float32)
    early, late = pl.pallas_call(
        functools.partial(kernel, blocks),
        out_shape=(out, out),
        in_specs=[pl.BlockSpec(memory_space=pltpu.HBM)] * 2,
        out_specs=(pl.BlockSpec(memory_space=pltpu.VMEM),) * 2,
        scratch_shapes=[
            pltpu.VMEM((ROWS, WIDTH), jnp.float32),
            pltpu.VMEM((4, 16, 128), jnp.int32),
            pltpu.VMEM((2, 4 * CHUNKS, WIDTH, LANES), jnp.bfloat16),
            pltpu.VMEM((3, ROWS, WIDTH), jnp.bfloat16),
            pltpu.VMEM((2, 16, 128), jnp.float32),
            pltpu.VMEM((3, ROWS, 128), jnp.float32),
            pltpu.VMEM((2, 4 * TILES, 8, 128), jnp.float32),
            pltpu.VMEM((3, ROWS, 128), jnp.float32),
            pltpu.VMEM((2, 4, 4, 128), jnp.float32),
            pltpu.VMEM((2, 4, 4, 128), jnp.float32),
            pltpu.VMEM((3, 4, 128), jnp.float32),
            pltpu.VMEM((3, 4, 128), jnp.float32),
            pltpu.SemaphoreType.DMA((ROWS // LOAD,)),
            pltpu.SemaphoreType.DMA((4,)),
            pltpu.SemaphoreType.DMA((9, max(PIECES, CHUNKS))),
            pltpu.SemaphoreType.DMA((9, max(PIECES, CHUNKS))),
            pltpu.SemaphoreType.REGULAR,
            pltpu.SemaphoreType.DMA((11,)),
            pltpu.SemaphoreType.DMA((11,)),
        ],
        compiler_params=pltpu.CompilerParams(
            collective_id=0, has_side_effects=True, vmem_limit_bytes=54976 << 10
        ),
    )(embeddings, ranks.reshape(-1, 128))

    def higher(one, other):
        return (jnp.maximum(one[0], other[0]), jnp.maximum(one[1], other[1]))

    start = jnp.float32(LOW)
    return lax.reduce(
        (early.reshape(2, -1), late.reshape(2, -1)), (start, start), higher, (0,)
    )


def solution(mesh):
    return jax.shard_map(
        functools.partial(shards, mesh.shape["blk"]),
        mesh=mesh,
        in_specs=(P(("blk", "rep"), None), P()),
        out_specs=(P(("blk", "rep")), P(("blk", "rep"))),
        check_vma=False,
    )
```

```python
import functools

import jax
import jax.numpy as jnp
from jax import lax
from jax.experimental import pallas as pl
from jax.experimental.pallas import tpu as pltpu
from jax.sharding import PartitionSpec as P

MESH = pl.DeviceIdType.MESH
ROWS = 512
WIDTH = 768
SIZES = (64, 192, 128, 128)
ENDS = tuple(sum(SIZES[: i + 1]) for i in range(len(SIZES)))
PIECES = len(SIZES)
EARLY = max(1, sum(end <= 256 for end in ENDS))
LOAD = 64
LANES = 128
CHUNKS = ROWS // LANES
TILES = ROWS // 128
NEAR = 3
LOW = -1.0

VIS, VIS2, UP, FAR, SIDE, PAIR, PAIR_SIDE, PAIR_UP, PAIR_FAR = range(9)


def kernel(
    blocks,
    emb_hbm,
    rank_hbm,
    early_ref,
    late_ref,
    emb,
    raw,
    host,
    visit,
    lane_rank,
    row_rank,
    host_best,
    visit_best,
    host_out,
    host_in,
    visit_out,
    visit_in,
    load_sem,
    rank_sem,
    send_sem,
    recv_sem,
    ready,
    relay,
    relay_sem,
    out_send,
    out_recv,
):
    b = lax.axis_index("blk")
    r = lax.axis_index("rep")
    y, c = r // 2, r % 2
    next_b, next_y = (b + 1) % blocks, (y + (b % 8) // 7) % 2
    prev_b, prev_y = (b + blocks - 1) % blocks, (y + (7 - b % 8) // 7) % 2
    back_b, back_y = (b + blocks - 2) % blocks, (prev_y + (7 - prev_b % 8) // 7) % 2
    ahead = (next_b, next_y * 2 + c)
    behind = (prev_b, prev_y * 2 + c)
    back = (back_b, back_y * 2 + c)
    side = (b, (1 - y) * 2 + c)
    pair = (b, y * 2 + 1 - c)
    place = b % 16
    over = ((b + blocks - 8) % blocks, (1 - y) * 2 + c)
    under = ((b + 8) % blocks, (1 - y) * 2 + c)

    def part(base_y, slot):
        return ((base_y + slot // 2) % 2) * 2 + (c + slot % 2) % 2

    def rows(i):
        return pl.ds(ENDS[i] - SIZES[i], SIZES[i])

    def copy(stream, i):
        if stream == VIS:
            src, dst, to = visit.at[0, rows(i)], visit.at[1, rows(i)], ahead
        elif stream == VIS2:
            src, dst, to = visit.at[1, rows(i)], visit.at[2, rows(i)], ahead
        elif stream == UP:
            src, dst, to = host.at[0, i], host.at[1, i], behind
        elif stream == FAR and i < NEAR:
            src, dst, to = host.at[1, i], host.at[1, 2 * CHUNKS + i], side
        elif stream == FAR:
            src, dst, to = host.at[0, 2 * CHUNKS + i], host.at[1, 2 * CHUNKS + i], behind
        elif stream == SIDE:
            src, dst, to = host.at[0, i], host.at[0, 2 * CHUNKS + i], side
        else:
            k = 0 if stream in (PAIR, PAIR_SIDE) else 1
            at = i if stream in (PAIR, PAIR_UP) else 2 * CHUNKS + i
            src, dst, to = host.at[k, at], host.at[k, at + CHUNKS], pair
        return pltpu.make_async_remote_copy(
            src_ref=src,
            dst_ref=dst,
            send_sem=send_sem.at[stream, i],
            recv_sem=recv_sem.at[stream, i],
            device_id=to,
            device_id_type=MESH,
        )

    def detour(src, dst, sent, got, to):
        return pltpu.make_async_remote_copy(
            src_ref=src,
            dst_ref=dst,
            send_sem=sent,
            recv_sem=got,
            device_id=to,
            device_id_type=MESH,
        )

    leave = detour(visit.at[1, rows(0)], relay, send_sem.at[VIS2, 0], relay_sem.at[1], over)
    along = detour(relay, relay, relay_sem.at[0], relay_sem.at[1], ahead)
    back_in = detour(
        relay, visit.at[2, rows(0)], relay_sem.at[0], recv_sem.at[VIS2, 0], under
    )

    started = []

    def send(stream, i):
        one = copy(stream, i)
        one.start()
        started.append(one)

    def arrived(stream, i):
        copy(stream, i).wait_recv()

    loads = [
        pltpu.make_async_copy(emb_hbm.at[at], emb.at[at], load_sem.at[i])
        for i, at in enumerate(pl.ds(n, LOAD) for n in range(0, ROWS, LOAD))
    ]
    for load in loads:
        load.start()

    barrier = pltpu.get_barrier_semaphore()
    for to in (behind, side, pair):
        pl.semaphore_signal(barrier, inc=1, device_id=to, device_id_type=MESH)

    rank_loads = [
        pltpu.make_async_copy(
            rank_hbm.at[pl.ds(pl.multiple_of(at * 16, 16), 16)], raw.at[k], rank_sem.at[k]
        )
        for k, at in enumerate((b, next_b, prev_b, back_b))
    ]
    for load in rank_loads:
        load.start()

    host_best[...] = jnp.full_like(host_best, LOW)
    visit_best[...] = jnp.full_like(visit_best, LOW)


    @pl.when(place == 6)
    def _():
        pl.semaphore_signal(barrier, inc=1, device_id=under, device_id_type=MESH)

    @pl.when(place == 15)
    def _():
        pl.semaphore_signal(barrier, inc=1, device_id=over, device_id_type=MESH)

    is_seventh = (place // 14) * (1 - place // 15)
    is_relay = (b % 8 // 7) * (1 - place // 8)
    pl.semaphore_wait(barrier, 3 + is_seventh + is_relay)
    pl.semaphore_signal(ready, inc=1, device_id=ahead, device_id_type=MESH)

    def first(j):
        for stream in (SIDE, PAIR):
            send(stream, j)

    for j in range(CHUNKS):
        group = []
        for at in range(j * LANES, (j + 1) * LANES, LOAD):
            loads[at // LOAD].wait()
            x = emb[pl.ds(at, LOAD), :]
            squares = jnp.sum(x * x, axis=1, keepdims=True)
            unit = x * lax.rsqrt(squares + 1e-06)
            visit[0, pl.ds(at, LOAD), :] = unit.astype(jnp.bfloat16)
            group.append(unit)
            if at in ENDS:
                send(VIS, ENDS.index(at))
        host[0, j] = jnp.concatenate(group, axis=0).T.astype(jnp.bfloat16)
        if j:
            first(j - 1)
    send(VIS, PIECES - 1)
    for load in rank_loads:
        load.wait()
    first(CHUNKS - 1)
    for k, base_y in ((0, y), (1, next_y)):
        for slot in range(4):
            lane_rank[k, pl.ds(slot * 4, 4), :] = raw[
                k, pl.ds(part(base_y, slot) * 4, 4), :
            ].astype(jnp.float32)
    for k, (at, base_y) in enumerate(((0, y), (2, prev_y), (3, back_y))):
        for t in range(4):
            line = raw[at, pl.ds(part(base_y, 0) * 4 + t, 1), :].astype(jnp.float32)
            row_rank[k, pl.ds(t * 128, 128), :] = jnp.broadcast_to(line, (128, 128)).T

    pl.semaphore_wait(ready, 1)
    for j in range(CHUNKS):
        send(UP, j)

    def meet(k, chunks, who, start=0, count=ROWS):
        scores = jnp.dot(
            visit[who, pl.ds(start, count), :],
            jnp.concatenate([host[k, n] for n in chunks], axis=1),
            preferred_element_type=jnp.float32,
        )
        before = row_rank[who, pl.ds(start, count), :]
        best = visit_best[who, pl.ds(start, count), :]
        for at, n in enumerate(chunks):
            after = lane_rank[k, pl.ds(n, 1), :]
            kept = jnp.where(before < after, scores[:, at * LANES : (at + 1) * LANES], LOW)
            best = jnp.maximum(best, kept)
            over = jnp.max(kept.reshape(count // 8, 8, LANES), axis=0)
            host_best[k, n] = jnp.maximum(host_best[k, n], over)
        visit_best[who, pl.ds(start, count), :] = best

    near = range(2 * CHUNKS)
    far = range(2 * CHUNKS, 4 * CHUNKS)
    lots = ((0, *range(NEAR, CHUNKS)), range(1, NEAR))
    far_lots = [[2 * CHUNKS + j + n for n in (0, CHUNKS) for j in lot] for lot in lots]

    def host_result(k, slot):
        for n in range(TILES):
            host_out[k, slot, pl.ds(n, 1), :] = jnp.max(
                host_best[k, slot * TILES + n], axis=0, keepdims=True
            )

    def visit_result(who, t):
        visit_out[who, pl.ds(t, 1), :] = jnp.max(
            visit_best[who, pl.ds(t * 128, 128), :].T, axis=0, keepdims=True
        )

    def host_copy(k, slot):
        return pltpu.make_async_remote_copy(
            src_ref=host_out.at[k, slot],
            dst_ref=host_in.at[k, slot],
            send_sem=out_send.at[k * 4 + slot],
            recv_sem=out_recv.at[k * 4 + slot],
            device_id=(b, part(y, slot)) if k == 0 else (next_b, part(next_y, slot)),
            device_id_type=MESH,
        )

    def visit_copy(who):
        return pltpu.make_async_remote_copy(
            src_ref=visit_out.at[who],
            dst_ref=visit_in.at[who],
            send_sem=out_send.at[8 + who],
            recv_sem=out_recv.at[8 + who],
            device_id=behind if who == 1 else back,
            device_id_type=MESH,
        )

    results = []

    def give(one):
        one.start()
        results.append(one)

    for j in range(CHUNKS):
        arrived(PAIR, j)
    meet(0, near, 0)
    for j in range(CHUNKS):
        for i in range(PIECES):
            if j * LANES < ENDS[i] <= (j + 1) * LANES:
                arrived(VIS, i)
                if i:
                    send(VIS2, i)
                    continue
                started.append(copy(VIS2, 0))

                @pl.when(place != 14)
                def _():
                    copy(VIS2, 0).start()

                @pl.when(place == 14)
                def _():
                    leave.start()
        arrived(SIDE, j)
        send(PAIR_SIDE, j)
        if j >= NEAR:
            send(FAR, j)
        if j == CHUNKS - 1:
            meet(0, near, 1)
            for n in range(CHUNKS):
                arrived(PAIR_SIDE, n)
            meet(0, far, 0)
            meet(0, far, 1)
        arrived(UP, j)
        send(PAIR_UP, j)
        if j < NEAR:
            send(FAR, j)
        if j == 0:

            @pl.when(place == 6)
            def _():
                along.wait_recv()
                along.start()
    for j in range(CHUNKS):
        arrived(PAIR_UP, j)
    meet(1, near, 1)
    for slot in range(4):
        host_result(0, slot)
    for t in range(4):
        visit_result(0, t)
    for slot in range(1, 4):
        give(host_copy(0, slot))

    @pl.when(place == 7)
    def _():
        along.wait_recv()
        back_in.start()

    for j in lots[0]:
        arrived(FAR, j)
        send(PAIR_FAR, j)
    for j in lots[0]:
        arrived(PAIR_FAR, j)
    meet(1, far_lots[0], 1)
    for n, j in enumerate(lots[1]):
        arrived(FAR, j)
        send(PAIR_FAR, j)
        if n == 0:
            for i in range(EARLY):
                arrived(VIS2, i)
            meet(1, near, 2, 0, ENDS[EARLY - 1])
            meet(1, far_lots[0], 2, 0, ENDS[EARLY - 1])
    for i in range(EARLY, PIECES - 1):
        arrived(VIS2, i)
        meet(1, near, 2, ENDS[i - 1], SIZES[i])
        meet(1, far_lots[0], 2, ENDS[i - 1], SIZES[i])
    before_last = ENDS[PIECES - 2]
    for j in lots[1]:
        arrived(PAIR_FAR, j)
    meet(1, far_lots[1], 1)
    meet(1, far_lots[1], 2, 0, before_last)
    arrived(VIS2, PIECES - 1)
    for which, chunks in ((1, far), (0, near)):
        meet(1, chunks, 2, before_last, ROWS - before_last)
        for slot in (2 * which, 2 * which + 1):
            host_result(1, slot)
        for slot in (2 * which, 2 * which + 1):
            give(host_copy(1, slot))
    for who in (2, 1):
        for t in range(4):
            visit_result(who, t)
        give(visit_copy(who))

    for one in started:
        one.wait_send()

    @pl.when((place == 6) | (place == 7))
    def _():
        along.wait_send()

    for one in results[:3]:
        one.wait_recv()
    early = host_out[0, 0]
    for slot in range(1, 4):
        early = jnp.maximum(early, host_in[0, slot])
    early_ref[0] = early
    for one in results[3:]:
        one.wait_recv()
    late_ref[0] = jnp.maximum(visit_out[0], visit_in[1])
    late_ref[1] = visit_in[2]
    early = host_in[1, 0]
    for slot in range(1, 4):
        early = jnp.maximum(early, host_in[1, slot])
    early_ref[1] = early
    for one in results:
        one.wait_send()


def shards(blocks, embeddings, ranks):
    out = jax.ShapeDtypeStruct((2, 4, 128), jnp.float32)
    early, late = pl.pallas_call(
        functools.partial(kernel, blocks),
        out_shape=(out, out),
        in_specs=[pl.BlockSpec(memory_space=pltpu.HBM)] * 2,
        out_specs=(pl.BlockSpec(memory_space=pltpu.VMEM),) * 2,
        scratch_shapes=[
            pltpu.VMEM((ROWS, WIDTH), jnp.float32),
            pltpu.VMEM((4, 16, 128), jnp.int32),
            pltpu.VMEM((2, 4 * CHUNKS, WIDTH, LANES), jnp.bfloat16),
            pltpu.VMEM((3, ROWS, WIDTH), jnp.bfloat16),
            pltpu.VMEM((2, 16, 128), jnp.float32),
            pltpu.VMEM((3, ROWS, 128), jnp.float32),
            pltpu.VMEM((2, 4 * TILES, 8, 128), jnp.float32),
            pltpu.VMEM((3, ROWS, 128), jnp.float32),
            pltpu.VMEM((2, 4, 4, 128), jnp.float32),
            pltpu.VMEM((2, 4, 4, 128), jnp.float32),
            pltpu.VMEM((3, 4, 128), jnp.float32),
            pltpu.VMEM((3, 4, 128), jnp.float32),
            pltpu.SemaphoreType.DMA((ROWS // LOAD,)),
            pltpu.SemaphoreType.DMA((4,)),
            pltpu.SemaphoreType.DMA((9, max(PIECES, CHUNKS))),
            pltpu.SemaphoreType.DMA((9, max(PIECES, CHUNKS))),
            pltpu.SemaphoreType.REGULAR,
            pltpu.VMEM((SIZES[0], WIDTH), jnp.bfloat16),
            pltpu.SemaphoreType.DMA((2,)),
            pltpu.SemaphoreType.DMA((11,)),
            pltpu.SemaphoreType.DMA((11,)),
        ],
        compiler_params=pltpu.CompilerParams(
            collective_id=0, has_side_effects=True, vmem_limit_bytes=54976 << 10
        ),
    )(embeddings, ranks.reshape(-1, 128))

    def higher(one, other):
        return (jnp.maximum(one[0], other[0]), jnp.maximum(one[1], other[1]))

    start = jnp.float32(LOW)
    return lax.reduce(
        (early.reshape(2, -1), late.reshape(2, -1)), (start, start), higher, (0,)
    )


def solution(mesh):
    return jax.shard_map(
        functools.partial(shards, mesh.shape["blk"]),
        mesh=mesh,
        in_specs=(P(("blk", "rep"), None), P()),
        out_specs=(P(("blk", "rep")), P(("blk", "rep"))),
        check_vma=False,
    )
```

```python
import functools

import jax
import jax.numpy as jnp
from jax import lax
from jax.experimental import pallas as pl
from jax.experimental.pallas import tpu as pltpu
from jax.sharding import PartitionSpec as P

MESH = pl.DeviceIdType.MESH
ROWS = 512
WIDTH = 768
SIZES = (64, 192, 128, 128)
ENDS = tuple(sum(SIZES[: i + 1]) for i in range(len(SIZES)))
PIECES = len(SIZES)
EARLY = max(1, sum(end <= 256 for end in ENDS))
LOAD = 64
LANES = 128
CHUNKS = ROWS // LANES
TILES = ROWS // 128
NEAR = 3
LOW = -1.0

VIS, VIS2, UP, FAR, SIDE, PAIR, PAIR_SIDE, PAIR_UP, PAIR_FAR = range(9)


def kernel(
    blocks,
    emb_hbm,
    rank_hbm,
    early_ref,
    late_ref,
    emb,
    raw,
    host,
    visit,
    lane_rank,
    row_rank,
    host_best,
    visit_best,
    host_out,
    host_in,
    visit_out,
    visit_in,
    load_sem,
    rank_sem,
    send_sem,
    recv_sem,
    ready,
    relay,
    relay_sem,
    out_send,
    out_recv,
):
    b = lax.axis_index("blk")
    r = lax.axis_index("rep")
    y, c = r // 2, r % 2
    next_b, next_y = (b + 1) % blocks, (y + (b % 8) // 7) % 2
    prev_b, prev_y = (b + blocks - 1) % blocks, (y + (7 - b % 8) // 7) % 2
    back_b, back_y = (b + blocks - 2) % blocks, (prev_y + (7 - prev_b % 8) // 7) % 2
    ahead = (next_b, next_y * 2 + c)
    behind = (prev_b, prev_y * 2 + c)
    back = (back_b, back_y * 2 + c)
    side = (b, (1 - y) * 2 + c)
    pair = (b, y * 2 + 1 - c)
    place = b % 16
    over = ((b + blocks - 8) % blocks, (1 - y) * 2 + c)
    under = ((b + 8) % blocks, (1 - y) * 2 + c)

    def part(base_y, slot):
        return ((base_y + slot // 2) % 2) * 2 + (c + slot % 2) % 2

    def rows(i):
        return pl.ds(ENDS[i] - SIZES[i], SIZES[i])

    def copy(stream, i):
        if stream == VIS:
            src, dst, to = visit.at[0, rows(i)], visit.at[1, rows(i)], ahead
        elif stream == VIS2:
            src, dst, to = visit.at[1, rows(i)], visit.at[2, rows(i)], ahead
        elif stream == UP:
            src, dst, to = host.at[0, i], host.at[1, i], behind
        elif stream == FAR and i < NEAR:
            src, dst, to = host.at[1, i], host.at[1, 2 * CHUNKS + i], side
        elif stream == FAR:
            src, dst, to = host.at[0, 2 * CHUNKS + i], host.at[1, 2 * CHUNKS + i], behind
        elif stream == SIDE:
            src, dst, to = host.at[0, i], host.at[0, 2 * CHUNKS + i], side
        else:
            k = 0 if stream in (PAIR, PAIR_SIDE) else 1
            at = i if stream in (PAIR, PAIR_UP) else 2 * CHUNKS + i
            src, dst, to = host.at[k, at], host.at[k, at + CHUNKS], pair
        return pltpu.make_async_remote_copy(
            src_ref=src,
            dst_ref=dst,
            send_sem=send_sem.at[stream, i],
            recv_sem=recv_sem.at[stream, i],
            device_id=to,
            device_id_type=MESH,
        )

    def detour(src, dst, sent, got, to):
        return pltpu.make_async_remote_copy(
            src_ref=src,
            dst_ref=dst,
            send_sem=sent,
            recv_sem=got,
            device_id=to,
            device_id_type=MESH,
        )

    leave = detour(visit.at[1, rows(0)], relay, send_sem.at[VIS2, 0], relay_sem.at[1], over)
    along = detour(relay, relay, relay_sem.at[0], relay_sem.at[1], ahead)
    back_in = detour(
        relay, visit.at[2, rows(0)], relay_sem.at[0], recv_sem.at[VIS2, 0], under
    )

    started = []

    def send(stream, i):
        one = copy(stream, i)
        one.start()
        started.append(one)

    def arrived(stream, i):
        copy(stream, i).wait_recv()

    loads = [
        pltpu.make_async_copy(emb_hbm.at[at], emb.at[at], load_sem.at[i])
        for i, at in enumerate(pl.ds(n, LOAD) for n in range(0, ROWS, LOAD))
    ]
    for load in loads:
        load.start()

    barrier = pltpu.get_barrier_semaphore()
    for to in (behind, side, pair):
        pl.semaphore_signal(barrier, inc=1, device_id=to, device_id_type=MESH)

    rank_loads = [
        pltpu.make_async_copy(
            rank_hbm.at[pl.ds(pl.multiple_of(at * 16, 16), 16)], raw.at[k], rank_sem.at[k]
        )
        for k, at in enumerate((b, next_b, prev_b, back_b))
    ]
    for load in rank_loads:
        load.start()

    host_best[...] = jnp.full_like(host_best, LOW)
    visit_best[...] = jnp.full_like(visit_best, LOW)


    @pl.when(place == 6)
    def _():
        pl.semaphore_signal(barrier, inc=1, device_id=under, device_id_type=MESH)

    @pl.when(place == 15)
    def _():
        pl.semaphore_signal(barrier, inc=1, device_id=over, device_id_type=MESH)

    is_seventh = (place // 14) * (1 - place // 15)
    is_relay = (b % 8 // 7) * (1 - place // 8)
    pl.semaphore_wait(barrier, 3 + is_seventh + is_relay)
    pl.semaphore_signal(ready, inc=1, device_id=ahead, device_id_type=MESH)

    def first(j):
        for stream in (SIDE, PAIR):
            send(stream, j)

    for j in range(CHUNKS):
        group = []
        for at in range(j * LANES, (j + 1) * LANES, LOAD):
            loads[at // LOAD].wait()
            x = emb[pl.ds(at, LOAD), :]
            squares = jnp.sum(x * x, axis=1, keepdims=True)
            unit = x * lax.rsqrt(squares + 1e-06)
            visit[0, pl.ds(at, LOAD), :] = unit.astype(jnp.bfloat16)
            group.append(unit)
            if at in ENDS:
                send(VIS, ENDS.index(at))
        host[0, j] = jnp.concatenate(group, axis=0).T.astype(jnp.bfloat16)
        if j:
            first(j - 1)
    send(VIS, PIECES - 1)
    for load in rank_loads:
        load.wait()
    first(CHUNKS - 1)
    for k, base_y in ((0, y), (1, next_y)):
        for slot in range(4):
            lane_rank[k, pl.ds(slot * 4, 4), :] = raw[
                k, pl.ds(part(base_y, slot) * 4, 4), :
            ].astype(jnp.float32)
    for k, (at, base_y) in enumerate(((0, y), (2, prev_y), (3, back_y))):
        for t in range(4):
            line = raw[at, pl.ds(part(base_y, 0) * 4 + t, 1), :].astype(jnp.float32)
            row_rank[k, pl.ds(t * 128, 128), :] = jnp.broadcast_to(line, (128, 128)).T

    pl.semaphore_wait(ready, 1)
    for j in range(CHUNKS):
        send(UP, j)

    def meet(k, chunks, who, start=0, count=ROWS):
        scores = jnp.dot(
            visit[who, pl.ds(start, count), :],
            jnp.concatenate([host[k, n] for n in chunks], axis=1),
            preferred_element_type=jnp.float32,
        )
        before = row_rank[who, pl.ds(start, count), :]
        best = visit_best[who, pl.ds(start, count), :]
        for at, n in enumerate(chunks):
            after = lane_rank[k, pl.ds(n, 1), :]
            kept = jnp.where(before < after, scores[:, at * LANES : (at + 1) * LANES], LOW)
            best = jnp.maximum(best, kept)
            over = jnp.max(kept.reshape(count // 8, 8, LANES), axis=0)
            host_best[k, n] = jnp.maximum(host_best[k, n], over)
        visit_best[who, pl.ds(start, count), :] = best

    near = range(2 * CHUNKS)
    far = range(2 * CHUNKS, 4 * CHUNKS)
    lots = ((0, *range(NEAR, CHUNKS)), range(1, NEAR))
    far_lots = [[2 * CHUNKS + j + n for n in (0, CHUNKS) for j in lot] for lot in lots]

    def host_result(k, slot):
        for n in range(TILES):
            host_out[k, slot, pl.ds(n, 1), :] = jnp.max(
                host_best[k, slot * TILES + n], axis=0, keepdims=True
            )

    def visit_result(who, t):
        visit_out[who, pl.ds(t, 1), :] = jnp.max(
            visit_best[who, pl.ds(t * 128, 128), :].T, axis=0, keepdims=True
        )

    def host_copy(k, slot):
        return pltpu.make_async_remote_copy(
            src_ref=host_out.at[k, slot],
            dst_ref=host_in.at[k, slot],
            send_sem=out_send.at[k * 4 + slot],
            recv_sem=out_recv.at[k * 4 + slot],
            device_id=(b, part(y, slot)) if k == 0 else (next_b, part(next_y, slot)),
            device_id_type=MESH,
        )

    def visit_copy(who):
        return pltpu.make_async_remote_copy(
            src_ref=visit_out.at[who],
            dst_ref=visit_in.at[who],
            send_sem=out_send.at[8 + who],
            recv_sem=out_recv.at[8 + who],
            device_id=behind if who == 1 else back,
            device_id_type=MESH,
        )

    results = []

    def give(one):
        one.start()
        results.append(one)

    for j in range(CHUNKS):
        arrived(PAIR, j)
    meet(0, near, 0)
    for j in range(CHUNKS):
        for i in range(PIECES):
            if j * LANES < ENDS[i] <= (j + 1) * LANES:
                arrived(VIS, i)
                if i:
                    send(VIS2, i)
                    continue
                started.append(copy(VIS2, 0))

                @pl.when(place != 14)
                def _():
                    copy(VIS2, 0).start()

                @pl.when(place == 14)
                def _():
                    leave.start()
        arrived(SIDE, j)
        send(PAIR_SIDE, j)
        if j >= NEAR:
            send(FAR, j)
        if j == CHUNKS - 1:
            meet(0, near, 1)
            for n in range(CHUNKS):
                arrived(PAIR_SIDE, n)
            meet(0, far, 0)
            meet(0, far, 1)
        arrived(UP, j)
        send(PAIR_UP, j)
        if j < NEAR:
            send(FAR, j)
        if j == 0:

            @pl.when(place == 6)
            def _():
                along.wait_recv()
                along.start()
    for j in range(CHUNKS):
        arrived(PAIR_UP, j)
    meet(1, near, 1)
    for slot in range(4):
        host_result(0, slot)
    for t in range(4):
        visit_result(0, t)
    for slot in range(1, 4):
        give(host_copy(0, slot))

    @pl.when(place == 7)
    def _():
        along.wait_recv()
        back_in.start()

    for j in lots[0]:
        arrived(FAR, j)
        send(PAIR_FAR, j)
    for j in lots[0]:
        arrived(PAIR_FAR, j)
    meet(1, far_lots[0], 1)
    for n, j in enumerate(lots[1]):
        arrived(FAR, j)
        send(PAIR_FAR, j)
        if n == 0:
            for i in range(EARLY):
                arrived(VIS2, i)
            meet(1, near, 2, 0, ENDS[EARLY - 1])
            meet(1, far_lots[0], 2, 0, ENDS[EARLY - 1])
    for i in range(EARLY, PIECES - 1):
        arrived(VIS2, i)
        meet(1, near, 2, ENDS[i - 1], SIZES[i])
        meet(1, far_lots[0], 2, ENDS[i - 1], SIZES[i])
    before_last = ENDS[PIECES - 2]
    for j in lots[1]:
        arrived(PAIR_FAR, j)
    meet(1, far_lots[1], 1)
    meet(1, far_lots[1], 2, 0, before_last)
    arrived(VIS2, PIECES - 1)
    for which, chunks in ((0, near), (1, far)):
        meet(1, chunks, 2, before_last, ROWS - before_last)
        for slot in (2 * which, 2 * which + 1):
            host_result(1, slot)
        for slot in (2 * which, 2 * which + 1):
            give(host_copy(1, slot))
    for who in (2, 1):
        for t in range(4):
            visit_result(who, t)
        give(visit_copy(who))

    for one in started:
        one.wait_send()

    @pl.when((place == 6) | (place == 7))
    def _():
        along.wait_send()

    for one in results[:3]:
        one.wait_recv()
    early = host_out[0, 0]
    for slot in range(1, 4):
        early = jnp.maximum(early, host_in[0, slot])
    early_ref[0] = early
    for one in results[3:]:
        one.wait_recv()
    late_ref[0] = jnp.maximum(visit_out[0], visit_in[1])
    late_ref[1] = visit_in[2]
    early = host_in[1, 0]
    for slot in range(1, 4):
        early = jnp.maximum(early, host_in[1, slot])
    early_ref[1] = early
    for one in results:
        one.wait_send()


def shards(blocks, embeddings, ranks):
    out = jax.ShapeDtypeStruct((2, 4, 128), jnp.float32)
    early, late = pl.pallas_call(
        functools.partial(kernel, blocks),
        out_shape=(out, out),
        in_specs=[pl.BlockSpec(memory_space=pltpu.HBM)] * 2,
        out_specs=(pl.BlockSpec(memory_space=pltpu.VMEM),) * 2,
        scratch_shapes=[
            pltpu.VMEM((ROWS, WIDTH), jnp.float32),
            pltpu.VMEM((4, 16, 128), jnp.int32),
            pltpu.VMEM((2, 4 * CHUNKS, WIDTH, LANES), jnp.bfloat16),
            pltpu.VMEM((3, ROWS, WIDTH), jnp.bfloat16),
            pltpu.VMEM((2, 16, 128), jnp.float32),
            pltpu.VMEM((3, ROWS, 128), jnp.float32),
            pltpu.VMEM((2, 4 * TILES, 8, 128), jnp.float32),
            pltpu.VMEM((3, ROWS, 128), jnp.float32),
            pltpu.VMEM((2, 4, 4, 128), jnp.float32),
            pltpu.VMEM((2, 4, 4, 128), jnp.float32),
            pltpu.VMEM((3, 4, 128), jnp.float32),
            pltpu.VMEM((3, 4, 128), jnp.float32),
            pltpu.SemaphoreType.DMA((ROWS // LOAD,)),
            pltpu.SemaphoreType.DMA((4,)),
            pltpu.SemaphoreType.DMA((9, max(PIECES, CHUNKS))),
            pltpu.SemaphoreType.DMA((9, max(PIECES, CHUNKS))),
            pltpu.SemaphoreType.REGULAR,
            pltpu.VMEM((SIZES[0], WIDTH), jnp.bfloat16),
            pltpu.SemaphoreType.DMA((2,)),
            pltpu.SemaphoreType.DMA((11,)),
            pltpu.SemaphoreType.DMA((11,)),
        ],
        compiler_params=pltpu.CompilerParams(
            collective_id=0, has_side_effects=True, vmem_limit_bytes=54976 << 10
        ),
    )(embeddings, ranks.reshape(-1, 128))

    def higher(one, other):
        return (jnp.maximum(one[0], other[0]), jnp.maximum(one[1], other[1]))

    start = jnp.float32(LOW)
    return lax.reduce(
        (early.reshape(2, -1), late.reshape(2, -1)), (start, start), higher, (0,)
    )


def solution(mesh):
    return jax.shard_map(
        functools.partial(shards, mesh.shape["blk"]),
        mesh=mesh,
        in_specs=(P(("blk", "rep"), None), P()),
        out_specs=(P(("blk", "rep")), P(("blk", "rep"))),
        check_vma=False,
    )
```

```python
import functools

import jax
import jax.numpy as jnp
from jax import lax
from jax.experimental import pallas as pl
from jax.experimental.pallas import tpu as pltpu
from jax.sharding import PartitionSpec as P

MESH = pl.DeviceIdType.MESH
ROWS = 512
WIDTH = 768
SIZES = (64, 192, 128, 128)
ENDS = tuple(sum(SIZES[: i + 1]) for i in range(len(SIZES)))
PIECES = len(SIZES)
EARLY = max(1, sum(end <= 256 for end in ENDS))
LOAD = 64
LANES = 128
CHUNKS = ROWS // LANES
TILES = ROWS // 128
NEAR = 3
LOW = -1.0

VIS, VIS2, UP, FAR, SIDE, PAIR, PAIR_SIDE, PAIR_UP, PAIR_FAR = range(9)


def kernel(
    blocks,
    emb_hbm,
    rank_hbm,
    early_ref,
    late_ref,
    emb,
    raw,
    host,
    visit,
    lane_rank,
    row_rank,
    host_best,
    visit_best,
    host_out,
    host_in,
    visit_out,
    visit_in,
    load_sem,
    rank_sem,
    send_sem,
    recv_sem,
    ready,
    relay,
    relay_sem,
    out_send,
    out_recv,
):
    b = lax.axis_index("blk")
    r = lax.axis_index("rep")
    y, c = r // 2, r % 2
    next_b, next_y = (b + 1) % blocks, (y + (b % 8) // 7) % 2
    prev_b, prev_y = (b + blocks - 1) % blocks, (y + (7 - b % 8) // 7) % 2
    back_b, back_y = (b + blocks - 2) % blocks, (prev_y + (7 - prev_b % 8) // 7) % 2
    ahead = (next_b, next_y * 2 + c)
    behind = (prev_b, prev_y * 2 + c)
    back = (back_b, back_y * 2 + c)
    side = (b, (1 - y) * 2 + c)
    pair = (b, y * 2 + 1 - c)
    place = b % 16
    over = ((b + blocks - 8) % blocks, (1 - y) * 2 + c)
    under = ((b + 8) % blocks, (1 - y) * 2 + c)

    def part(base_y, slot):
        return ((base_y + slot // 2) % 2) * 2 + (c + slot % 2) % 2

    def rows(i):
        return pl.ds(ENDS[i] - SIZES[i], SIZES[i])

    def copy(stream, i):
        if stream == VIS:
            src, dst, to = visit.at[0, rows(i)], visit.at[1, rows(i)], ahead
        elif stream == VIS2:
            src, dst, to = visit.at[1, rows(i)], visit.at[2, rows(i)], ahead
        elif stream == UP:
            src, dst, to = host.at[0, i], host.at[1, i], behind
        elif stream == FAR and i < NEAR:
            src, dst, to = host.at[1, i], host.at[1, 2 * CHUNKS + i], side
        elif stream == FAR:
            src, dst, to = host.at[0, 2 * CHUNKS + i], host.at[1, 2 * CHUNKS + i], behind
        elif stream == SIDE:
            src, dst, to = host.at[0, i], host.at[0, 2 * CHUNKS + i], side
        else:
            k = 0 if stream in (PAIR, PAIR_SIDE) else 1
            at = i if stream in (PAIR, PAIR_UP) else 2 * CHUNKS + i
            src, dst, to = host.at[k, at], host.at[k, at + CHUNKS], pair
        return pltpu.make_async_remote_copy(
            src_ref=src,
            dst_ref=dst,
            send_sem=send_sem.at[stream, i],
            recv_sem=recv_sem.at[stream, i],
            device_id=to,
            device_id_type=MESH,
        )

    def detour(src, dst, sent, got, to):
        return pltpu.make_async_remote_copy(
            src_ref=src,
            dst_ref=dst,
            send_sem=sent,
            recv_sem=got,
            device_id=to,
            device_id_type=MESH,
        )

    leave = detour(visit.at[1, rows(0)], relay, send_sem.at[VIS2, 0], relay_sem.at[1], over)
    along = detour(relay, relay, relay_sem.at[0], relay_sem.at[1], ahead)
    back_in = detour(
        relay, visit.at[2, rows(0)], relay_sem.at[0], recv_sem.at[VIS2, 0], under
    )

    started = []

    def send(stream, i):
        one = copy(stream, i)
        one.start()
        started.append(one)

    def arrived(stream, i):
        copy(stream, i).wait_recv()

    loads = [
        pltpu.make_async_copy(emb_hbm.at[at], emb.at[at], load_sem.at[i])
        for i, at in enumerate(pl.ds(n, LOAD) for n in range(0, ROWS, LOAD))
    ]
    for load in loads:
        load.start()

    barrier = pltpu.get_barrier_semaphore()
    for to in (behind, side, pair):
        pl.semaphore_signal(barrier, inc=1, device_id=to, device_id_type=MESH)

    rank_loads = [
        pltpu.make_async_copy(
            rank_hbm.at[pl.ds(pl.multiple_of(at * 16, 16), 16)], raw.at[k], rank_sem.at[k]
        )
        for k, at in enumerate((b, next_b, prev_b, back_b))
    ]
    for load in rank_loads:
        load.start()

    host_best[...] = jnp.full_like(host_best, LOW)
    visit_best[...] = jnp.full_like(visit_best, LOW)


    @pl.when(place == 6)
    def _():
        pl.semaphore_signal(barrier, inc=1, device_id=under, device_id_type=MESH)

    @pl.when(place == 15)
    def _():
        pl.semaphore_signal(barrier, inc=1, device_id=over, device_id_type=MESH)

    is_seventh = (place // 14) * (1 - place // 15)
    is_relay = (b % 8 // 7) * (1 - place // 8)
    pl.semaphore_wait(barrier, 3 + is_seventh + is_relay)
    pl.semaphore_signal(ready, inc=1, device_id=ahead, device_id_type=MESH)

    def first(j):
        for stream in (SIDE, PAIR):
            send(stream, j)

    for j in range(CHUNKS):
        group = []
        for at in range(j * LANES, (j + 1) * LANES, LOAD):
            loads[at // LOAD].wait()
            x = emb[pl.ds(at, LOAD), :]
            squares = jnp.sum(x * x, axis=1, keepdims=True)
            unit = x * lax.rsqrt(squares + 1e-06)
            visit[0, pl.ds(at, LOAD), :] = unit.astype(jnp.bfloat16)
            group.append(unit)
            if at in ENDS:
                send(VIS, ENDS.index(at))
        host[0, j] = jnp.concatenate(group, axis=0).T.astype(jnp.bfloat16)
        if j:
            first(j - 1)
    send(VIS, PIECES - 1)
    for load in rank_loads:
        load.wait()
    first(CHUNKS - 1)
    pl.semaphore_wait(ready, 1)
    for j in range(CHUNKS):
        send(UP, j)

    for k, base_y in ((0, y), (1, next_y)):
        for slot in range(4):
            lane_rank[k, pl.ds(slot * 4, 4), :] = raw[
                k, pl.ds(part(base_y, slot) * 4, 4), :
            ].astype(jnp.float32)
    for k, (at, base_y) in enumerate(((0, y), (2, prev_y), (3, back_y))):
        for t in range(4):
            line = raw[at, pl.ds(part(base_y, 0) * 4 + t, 1), :].astype(jnp.float32)
            row_rank[k, pl.ds(t * 128, 128), :] = jnp.broadcast_to(line, (128, 128)).T

    def meet(k, chunks, who, start=0, count=ROWS):
        scores = jnp.dot(
            visit[who, pl.ds(start, count), :],
            jnp.concatenate([host[k, n] for n in chunks], axis=1),
            preferred_element_type=jnp.float32,
        )
        before = row_rank[who, pl.ds(start, count), :]
        best = visit_best[who, pl.ds(start, count), :]
        for at, n in enumerate(chunks):
            after = lane_rank[k, pl.ds(n, 1), :]
            kept = jnp.where(before < after, scores[:, at * LANES : (at + 1) * LANES], LOW)
            best = jnp.maximum(best, kept)
            over = jnp.max(kept.reshape(count // 8, 8, LANES), axis=0)
            host_best[k, n] = jnp.maximum(host_best[k, n], over)
        visit_best[who, pl.ds(start, count), :] = best

    near = range(2 * CHUNKS)
    far = range(2 * CHUNKS, 4 * CHUNKS)
    lots = ((0, *range(NEAR, CHUNKS)), range(1, NEAR))
    far_lots = [[2 * CHUNKS + j + n for n in (0, CHUNKS) for j in lot] for lot in lots]

    def host_result(k, slot):
        for n in range(TILES):
            host_out[k, slot, pl.ds(n, 1), :] = jnp.max(
                host_best[k, slot * TILES + n], axis=0, keepdims=True
            )

    def visit_result(who, t):
        visit_out[who, pl.ds(t, 1), :] = jnp.max(
            visit_best[who, pl.ds(t * 128, 128), :].T, axis=0, keepdims=True
        )

    def host_copy(k, slot):
        return pltpu.make_async_remote_copy(
            src_ref=host_out.at[k, slot],
            dst_ref=host_in.at[k, slot],
            send_sem=out_send.at[k * 4 + slot],
            recv_sem=out_recv.at[k * 4 + slot],
            device_id=(b, part(y, slot)) if k == 0 else (next_b, part(next_y, slot)),
            device_id_type=MESH,
        )

    def visit_copy(who):
        return pltpu.make_async_remote_copy(
            src_ref=visit_out.at[who],
            dst_ref=visit_in.at[who],
            send_sem=out_send.at[8 + who],
            recv_sem=out_recv.at[8 + who],
            device_id=behind if who == 1 else back,
            device_id_type=MESH,
        )

    results = []

    def give(one):
        one.start()
        results.append(one)

    for j in range(CHUNKS):
        arrived(PAIR, j)
    meet(0, near, 0)
    for j in range(CHUNKS):
        for i in range(PIECES):
            if j * LANES < ENDS[i] <= (j + 1) * LANES:
                arrived(VIS, i)
                if i:
                    send(VIS2, i)
                    continue
                started.append(copy(VIS2, 0))

                @pl.when(place != 14)
                def _():
                    copy(VIS2, 0).start()

                @pl.when(place == 14)
                def _():
                    leave.start()
        arrived(SIDE, j)
        send(PAIR_SIDE, j)
        if j >= NEAR:
            send(FAR, j)
        if j == CHUNKS - 1:
            meet(0, near, 1)
            for n in range(CHUNKS):
                arrived(PAIR_SIDE, n)
            meet(0, far, 0)
            meet(0, far, 1)
        arrived(UP, j)
        send(PAIR_UP, j)
        if j < NEAR:
            send(FAR, j)
        if j == 0:

            @pl.when(place == 6)
            def _():
                along.wait_recv()
                along.start()
    for j in range(CHUNKS):
        arrived(PAIR_UP, j)
    meet(1, near, 1)
    for slot in range(4):
        host_result(0, slot)
    for t in range(4):
        visit_result(0, t)
    for slot in range(1, 4):
        give(host_copy(0, slot))

    @pl.when(place == 7)
    def _():
        along.wait_recv()
        back_in.start()

    for j in lots[0]:
        arrived(FAR, j)
        send(PAIR_FAR, j)
    for j in lots[0]:
        arrived(PAIR_FAR, j)
    meet(1, far_lots[0], 1)
    for n, j in enumerate(lots[1]):
        arrived(FAR, j)
        send(PAIR_FAR, j)
        if n == 0:
            for i in range(EARLY):
                arrived(VIS2, i)
            meet(1, near, 2, 0, ENDS[EARLY - 1])
            meet(1, far_lots[0], 2, 0, ENDS[EARLY - 1])
    for i in range(EARLY, PIECES - 1):
        arrived(VIS2, i)
        meet(1, near, 2, ENDS[i - 1], SIZES[i])
        meet(1, far_lots[0], 2, ENDS[i - 1], SIZES[i])
    before_last = ENDS[PIECES - 2]
    for j in lots[1]:
        arrived(PAIR_FAR, j)
    meet(1, far_lots[1], 1)
    meet(1, far_lots[1], 2, 0, before_last)
    arrived(VIS2, PIECES - 1)
    for which, chunks in ((0, near), (1, far)):
        meet(1, chunks, 2, before_last, ROWS - before_last)
        for slot in (2 * which, 2 * which + 1):
            host_result(1, slot)
        for slot in (2 * which, 2 * which + 1):
            give(host_copy(1, slot))
    for who in (2, 1):
        for t in range(4):
            visit_result(who, t)
        give(visit_copy(who))

    for one in started:
        one.wait_send()

    @pl.when((place == 6) | (place == 7))
    def _():
        along.wait_send()

    for one in results[:3]:
        one.wait_recv()
    early = host_out[0, 0]
    for slot in range(1, 4):
        early = jnp.maximum(early, host_in[0, slot])
    early_ref[0] = early
    for one in results[3:]:
        one.wait_recv()
    late_ref[0] = jnp.maximum(visit_out[0], visit_in[1])
    late_ref[1] = visit_in[2]
    early = host_in[1, 0]
    for slot in range(1, 4):
        early = jnp.maximum(early, host_in[1, slot])
    early_ref[1] = early
    for one in results:
        one.wait_send()


def shards(blocks, embeddings, ranks):
    out = jax.ShapeDtypeStruct((2, 4, 128), jnp.float32)
    early, late = pl.pallas_call(
        functools.partial(kernel, blocks),
        out_shape=(out, out),
        in_specs=[pl.BlockSpec(memory_space=pltpu.HBM)] * 2,
        out_specs=(pl.BlockSpec(memory_space=pltpu.VMEM),) * 2,
        scratch_shapes=[
            pltpu.VMEM((ROWS, WIDTH), jnp.float32),
            pltpu.VMEM((4, 16, 128), jnp.int32),
            pltpu.VMEM((2, 4 * CHUNKS, WIDTH, LANES), jnp.bfloat16),
            pltpu.VMEM((3, ROWS, WIDTH), jnp.bfloat16),
            pltpu.VMEM((2, 16, 128), jnp.float32),
            pltpu.VMEM((3, ROWS, 128), jnp.float32),
            pltpu.VMEM((2, 4 * TILES, 8, 128), jnp.float32),
            pltpu.VMEM((3, ROWS, 128), jnp.float32),
            pltpu.VMEM((2, 4, 4, 128), jnp.float32),
            pltpu.VMEM((2, 4, 4, 128), jnp.float32),
            pltpu.VMEM((3, 4, 128), jnp.float32),
            pltpu.VMEM((3, 4, 128), jnp.float32),
            pltpu.SemaphoreType.DMA((ROWS // LOAD,)),
            pltpu.SemaphoreType.DMA((4,)),
            pltpu.SemaphoreType.DMA((9, max(PIECES, CHUNKS))),
            pltpu.SemaphoreType.DMA((9, max(PIECES, CHUNKS))),
            pltpu.SemaphoreType.REGULAR,
            pltpu.VMEM((SIZES[0], WIDTH), jnp.bfloat16),
            pltpu.SemaphoreType.DMA((2,)),
            pltpu.SemaphoreType.DMA((11,)),
            pltpu.SemaphoreType.DMA((11,)),
        ],
        compiler_params=pltpu.CompilerParams(
            collective_id=0, has_side_effects=True, vmem_limit_bytes=54976 << 10
        ),
    )(embeddings, ranks.reshape(-1, 128))

    def higher(one, other):
        return (jnp.maximum(one[0], other[0]), jnp.maximum(one[1], other[1]))

    start = jnp.float32(LOW)
    return lax.reduce(
        (early.reshape(2, -1), late.reshape(2, -1)), (start, start), higher, (0,)
    )


def solution(mesh):
    return jax.shard_map(
        functools.partial(shards, mesh.shape["blk"]),
        mesh=mesh,
        in_specs=(P(("blk", "rep"), None), P()),
        out_specs=(P(("blk", "rep")), P(("blk", "rep"))),
        check_vma=False,
    )
```
